256 devices in a mesh: dev: 128 (over y, x, z), rep: 2 (over core).
Axes of the slice: x: 4, y: 4, z: 8, core: 2. Of those that a mesh axis runs over, the one named last changes fastest.
Arguments:
- embeddings: float32 [32768, 4096], P(('rep', 'dev')), parts along dimension 0, may hold values from -130 to 130
- cluster_id: int32 [32768], P(('rep', 'dev')), parts along dimension 0, may hold values from 0 to 255, as said below
- member_order: int32 [32768], P(('rep', 'dev')), parts along dimension 0, may hold values from 0 to 127, as said below
- cluster_slot: int32 [512], P('rep'), parts along dimension 0, may hold values from 0 to 255, each once
- cluster_size: int32 [512], P('rep'), parts along dimension 0, may hold values from 16 to 128, as said below
Outputs:
- best_similarity: float32 [32768], P(('rep', 'dev')), parts along dimension 0
- keep: int32 [32768], P(('rep', 'dev')), parts along dimension 0
- cluster_mean: float32 [512], P(('rep', 'dev')), parts along dimension 0
The draws below stay inside these ranges and needn't reach their ends.
There are 2 independent parts, one for each index of `rep`. The reference program is written for one: setup_inputs(seed, part) draws one part's arguments, and reference() takes and returns one part's arrays. A program takes and returns all parts, laid end to end along the dimension named above; each array names one. Nothing has to cross between parts.
Inputs may be any that keep to these rules, and one draw needn't show every extreme that they name: `cluster_id`: every cluster holds at most 128 rows and some cluster exactly 128. A cluster of n members has floor(n / 128) or ceil(n / 128) of them among the rows of each device, so at most 1, a number reached on every device. `member_order`: within a cluster of n members the ranks are 0 to n - 1, each once. `cluster_slot`: a permutation; cluster c is owned by device cluster_slot[c] // 2 of dev. `cluster_size`: the number of rows whose cluster_id is c.
All inputs are finite; a program needn't handle non-finite values.
Results may differ from the reference program's by a relative error of at most 0.0003.
Values may be sent and summed in bfloat16 or wider, within the bound.
No kernel may reach another device: no remote copies, remote signals or barrier semaphores. Data moves between devices by JAX's collectives and lax.ppermute only.
A program may use at most 64 MiB of HBM per device.

```python
import jax
import jax.numpy as jnp
from jax import lax

D = 4096
CAP = 128
CLUSTERS = 256
ROWS_ALL = 16384
N_DEV = 128


def layout(key):
    base_key = jax.random.fold_in(key, 7)
    key_sizes, key_labels, key_order, key_source, key_rows = jax.random.split(base_key, 5)
    half_count = CLUSTERS // 2
    sizes_pair = jax.random.randint(key_sizes, (half_count,), CAP // 8, CAP - CAP // 8 + 1)
    base_sizes = jnp.concatenate([sizes_pair, CAP - sizes_pair]).astype(jnp.int32)
    base_sizes = base_sizes.at[0].set(CAP).at[half_count].set(CAP // 2).at[1].set(CAP // 4).at[half_count + 1].set(CAP // 4)
    labels = jax.random.permutation(key_labels, CLUSTERS)
    sizes_out = jnp.zeros((CLUSTERS,), jnp.int32).at[labels].set(base_sizes)
    size_ends = jnp.cumsum(sizes_out)
    size_starts = size_ends - sizes_out
    positions = jnp.arange(ROWS_ALL, dtype=jnp.int32)
    owner_cluster = jnp.sum((positions[:, None] >= size_ends[None, :]).astype(jnp.int32), axis=1)
    shuffle = jax.random.permutation(key_order, ROWS_ALL).astype(jnp.int32)
    ranked = jnp.argsort(owner_cluster * ROWS_ALL + shuffle, stable=True)
    inverse = jnp.zeros((ROWS_ALL,), jnp.int32).at[ranked].set(positions)
    orders = inverse - size_starts[owner_cluster]
    source_perm = jax.random.permutation(key_source, N_DEV).astype(jnp.int32)
    source = source_perm[positions % N_DEV]
    second = jax.random.permutation(key_rows, ROWS_ALL).astype(jnp.int32)
    placed = jnp.argsort(source * ROWS_ALL + second, stable=True)
    target = jnp.zeros((ROWS_ALL,), jnp.int32).at[placed].set(positions)
    ids_out = jnp.zeros((ROWS_ALL,), jnp.int32).at[target].set(owner_cluster)
    order_out = jnp.zeros((ROWS_ALL,), jnp.int32).at[target].set(orders)
    return (ids_out, order_out, sizes_out)


def draw_cluster_id(key, part):
    return layout(key)[0]


def draw_member_order(key, part):
    return layout(key)[1]


def draw_cluster_size(key, part):
    return layout(key)[2]


def draw_embeddings(key, part):
    cluster_ids = layout(key)[0]
    base_key = jax.random.fold_in(key, 11)
    key_anchor, key_noise, key_copy = jax.random.split(base_key, 3)
    anchors = jnp.clip(jax.random.normal(key_anchor, (CLUSTERS, D), jnp.float32), -8.0, 8.0)
    noise = jnp.clip(jax.random.normal(key_noise, (ROWS_ALL, D), jnp.float32), -8.0, 8.0)
    copied = jax.random.randint(key_copy, (ROWS_ALL,), 0, 3) == 0
    values = jnp.where(copied[:, None], anchors[cluster_ids] + 0.15 * noise, noise)
    return values.astype(jnp.float32)


def setup_inputs(seed: int = 0, part: int = 0) -> dict:
    key_list = jax.random.split(jax.random.key(seed), 6)
    own_keys = jax.random.split(jax.random.fold_in(key_list[5], part), 6)
    embeddings = draw_embeddings(jax.random.fold_in(jax.random.fold_in(key_list[5], part), 71), part)
    cluster_id = draw_cluster_id(jax.random.fold_in(jax.random.fold_in(key_list[5], part), 71), part)
    member_order = draw_member_order(jax.random.fold_in(jax.random.fold_in(key_list[5], part), 71), part)
    cluster_slot = jax.random.permutation(own_keys[3], CLUSTERS).astype(jnp.int32)
    cluster_size = draw_cluster_size(jax.random.fold_in(jax.random.fold_in(key_list[5], part), 71), part)
    return {"embeddings": embeddings, "cluster_id": cluster_id, "member_order": member_order, "cluster_slot": cluster_slot, "cluster_size": cluster_size}


norm_eps = 1e-06
cutoff = 0.8

def normalized(values):
    squares_sum = lax.optimization_barrier(jnp.sum(values * values, axis=1, keepdims=True))
    return (values * lax.rsqrt(squares_sum + norm_eps)).astype(jnp.bfloat16)

def reference(embeddings, cluster_id, member_order, cluster_slot, cluster_size):
    unit_rows = normalized(embeddings)
    total_rows = embeddings.shape[0]
    where_put = (cluster_id * CAP + member_order).astype(jnp.int32)
    index_table = jnp.zeros((CLUSTERS * CAP,), jnp.int32).at[where_put].set(jnp.arange(total_rows, dtype=jnp.int32) + 1).reshape(CLUSTERS, CAP)
    spot_index = jnp.arange(CAP, dtype=jnp.int32)
    lower = spot_index[None, :] < spot_index[:, None]

    def one_cluster(packed):
        entries, size_now = packed
        occupied = entries > 0
        gathered = unit_rows[jnp.maximum(entries - 1, 0)].astype(jnp.float32)
        members = jnp.where(occupied[:, None], gathered, 0.0)
        is_live = occupied & (spot_index < size_now)
        similar = jnp.dot(members, members.T, preferred_element_type=jnp.float32)
        allowed = lower & is_live[None, :]
        nearest = lax.optimization_barrier(jnp.max(jnp.where(allowed, similar, -1.0), axis=1))
        best_spot = jnp.where(is_live, nearest, -1.0)
        mean_best = jnp.sum(jnp.where(is_live, best_spot, 0.0)) / size_now.astype(jnp.float32)
        return (best_spot, mean_best)
    best_table, cluster_means = lax.map(one_cluster, (index_table, cluster_size))
    row_best = best_table.reshape(-1)[where_put]
    keep_mask = (row_best < cutoff).astype(jnp.int32)
    by_slot = jnp.zeros((CLUSTERS,), jnp.float32).at[cluster_slot].set(cluster_means)
    return (row_best, keep_mask, by_slot)
```

```python
import jax
import jax.numpy as jnp
from jax import lax
from jax.experimental import pallas as pl
from jax.experimental.pallas import tpu as pltpu
from jax.sharding import PartitionSpec as P

CAP = 128
LANES = 128

norm_eps = 1e-06
cutoff = 0.8


def iota(shape, axis):
    return lax.broadcasted_iota(jnp.int32, shape, axis)


def table_lookup(cluster_row, table_row):
    clusters = table_row.shape[1]
    hit = (iota((clusters, cluster_row.shape[1]), 0) == cluster_row).astype(jnp.bfloat16)
    table = jnp.broadcast_to(table_row.astype(jnp.bfloat16), (8, clusters))
    return jnp.dot(table, hit, preferred_element_type=jnp.float32)[:1]


def place_kernel(emb_ref, id_ref, order_ref, slot_ref, size_ref, out_ref, where_ref):
    values = emb_ref[...]
    squares_sum = jnp.sum(values * values, axis=1, keepdims=True)
    unit = (values * lax.rsqrt(squares_sum + norm_eps)).astype(jnp.bfloat16)
    ids = id_ref[...]
    slot_of = table_lookup(ids, slot_ref[...]).astype(jnp.int32)
    size_of = table_lookup(ids, size_ref[...]).astype(jnp.int32)
    order = order_ref[...]
    code = jnp.where(order < size_of, order + 1, 0).astype(jnp.float32)
    slots = out_ref.shape[0]
    depth = values.shape[1]
    hit = iota((slots, values.shape[0]), 0) == slot_of
    out_ref[:, :depth] = jnp.dot(
        hit.astype(jnp.bfloat16), unit, preferred_element_type=jnp.float32
    ).astype(jnp.bfloat16)
    rank = jnp.sum(jnp.where(hit, code, 0.0), axis=1, keepdims=True)
    out_ref[:, depth:] = jnp.broadcast_to(rank, (slots, LANES)).astype(jnp.bfloat16)
    where_ref[...] = slot_of


def best_kernel(got_ref, slot_ref, size_ref, best_ref, mean_ref, spread_ref):
    rows = got_ref.shape[0]
    depth = got_ref.shape[1] - LANES
    unit = got_ref[:, :depth]
    coded = got_ref[:, depth:]
    similar = lax.dot_general(
        unit, unit, (((1,), (1,)), ((), ())), preferred_element_type=jnp.float32
    )
    rank_col = coded.astype(jnp.float32)[:, :1]
    first = (iota((8, LANES), 1) == 0).astype(jnp.bfloat16)
    rank_row = lax.dot_general(
        first, coded, (((1,), (1,)), ((), ())), preferred_element_type=jnp.float32
    )[:1]
    same = ((iota((rows, rows), 0) ^ iota((rows, rows), 1)) & 1) == 0
    allowed = same & (rank_row > 0.0) & (rank_row < rank_col)
    best = jnp.max(jnp.where(allowed, similar, -1.0), axis=1, keepdims=True)
    spread_ref[...] = jnp.broadcast_to(best, spread_ref.shape)
    live_col = jnp.broadcast_to(rank_col, spread_ref.shape) > 0.0
    summed = jnp.where(live_col, spread_ref[...], 0.0)
    odd = (iota(spread_ref.shape, 0) & 1) == 1
    lane = iota((1, LANES), 1)
    total = jnp.where(
        lane == 0,
        jnp.sum(jnp.where(odd, 0.0, summed), axis=0, keepdims=True),
        jnp.sum(jnp.where(odd, summed, 0.0), axis=0, keepdims=True),
    )
    half = rows // 2
    even_best = spread_ref[pl.ds(0, half, stride=2), :]
    odd_best = spread_ref[pl.ds(1, half, stride=2), :]
    best_ref[...] = jnp.where(iota((half, LANES), 1) == 0, even_best, odd_best)
    first_slot = lax.axis_index("dev") * 2
    slots = slot_ref[...]
    sizes = size_ref[...]
    size0 = jnp.sum(jnp.where(slots == first_slot, sizes, 0), axis=1, keepdims=True)
    size1 = jnp.sum(jnp.where(slots == first_slot + 1, sizes, 0), axis=1, keepdims=True)
    size = jnp.where(lane == 0, size0, size1)
    mean_ref[...] = total / size.astype(jnp.float32)


def pick_kernel(back_ref, where_ref, best_ref, keep_ref):
    slot_of = where_ref[...]
    back = back_ref[...]
    owners = iota((back.shape[0], slot_of.shape[1]), 0)
    from_even = jnp.where(owners * 2 == slot_of, back[:, :1], 0.0)
    from_odd = jnp.where(owners * 2 + 1 == slot_of, back[:, 1:2], 0.0)
    best = jnp.sum(from_even + from_odd, axis=0, keepdims=True)
    best_ref[...] = best
    keep_ref[...] = (best < cutoff).astype(jnp.int32)


def body(embeddings, cluster_id, member_order, cluster_slot, cluster_size):
    devices = lax.axis_size("dev")
    rows, depth = embeddings.shape
    clusters = cluster_slot.shape[0]
    ids = cluster_id.reshape(1, rows)
    order = member_order.reshape(1, rows)
    slot = cluster_slot.reshape(1, clusters)
    size = cluster_size.reshape(1, clusters)
    width = depth + LANES
    payload, place = pl.pallas_call(
        place_kernel,
        out_shape=(
            jax.ShapeDtypeStruct((clusters, width), jnp.bfloat16),
            jax.ShapeDtypeStruct((1, rows), jnp.int32),
        ),
        name="place",
    )(embeddings, ids, order, slot, size)
    got = lax.all_to_all(payload, "dev", split_axis=0, concat_axis=0, tiled=True)
    best, mean = pl.pallas_call(
        best_kernel,
        out_shape=(
            jax.ShapeDtypeStruct((devices, LANES), jnp.float32),
            jax.ShapeDtypeStruct((1, LANES), jnp.float32),
        ),
        scratch_shapes=[pltpu.VMEM((clusters, LANES), jnp.float32)],
        name="best",
    )(got, slot, size)
    back = lax.all_to_all(
        best.reshape(devices, 1, LANES), "dev", split_axis=0, concat_axis=0, tiled=True
    ).reshape(devices, LANES)
    row_best, keep = pl.pallas_call(
        pick_kernel,
        out_shape=(
            jax.ShapeDtypeStruct((1, rows), jnp.float32),
            jax.ShapeDtypeStruct((1, rows), jnp.int32),
        ),
        name="pick",
    )(back, place)
    return (row_best.reshape(rows), keep.reshape(rows), mean[0, :2])


def solution(mesh):
    placed = (P(("rep", "dev"), None), P(("rep", "dev")), P(("rep", "dev")), P("rep"), P("rep"))
    return jax.shard_map(
        body,
        mesh=mesh,
        in_specs=placed,
        out_specs=(P(("rep", "dev")), P(("rep", "dev")), P(("rep", "dev"))),
        check_vma=False,
    )
```

```python
import jax
import jax.numpy as jnp
from jax import lax
from jax.experimental import pallas as pl
from jax.experimental.pallas import tpu as pltpu
from jax.sharding import PartitionSpec as P

CAP = 128
LANES = 128

norm_eps = 1e-06
cutoff = 0.8


def iota(shape, axis):
    return lax.broadcasted_iota(jnp.int32, shape, axis)


def table_lookup(cluster_row, table_row):
    clusters = table_row.shape[1]
    hit = (iota((clusters, cluster_row.shape[1]), 0) == cluster_row).astype(jnp.bfloat16)
    table = jnp.broadcast_to(table_row.astype(jnp.bfloat16), (8, clusters))
    return jnp.dot(table, hit, preferred_element_type=jnp.float32)[:1]


def place_kernel(emb_ref, id_ref, order_ref, slot_ref, size_ref, out_ref, where_ref):
    values = emb_ref[...]
    squares_sum = jnp.sum(values * values, axis=1, keepdims=True)
    unit = (values * lax.rsqrt(squares_sum + norm_eps)).astype(jnp.bfloat16)
    ids = id_ref[...]
    slot_of = table_lookup(ids, slot_ref[...]).astype(jnp.int32)
    size_of = table_lookup(ids, size_ref[...]).astype(jnp.int32)
    order = order_ref[...]
    code = jnp.where(order < size_of, order + 1, 0).astype(jnp.float32)
    slots = out_ref.shape[0]
    depth = values.shape[1]
    hit = iota((slots, values.shape[0]), 0) == slot_of
    out_ref[:, :depth] = jnp.dot(
        hit.astype(jnp.bfloat16), unit, preferred_element_type=jnp.float32
    ).astype(jnp.bfloat16)
    rank = jnp.sum(jnp.where(hit, code, 0.0), axis=1, keepdims=True)
    out_ref[:, depth:] = jnp.broadcast_to(rank, (slots, LANES)).astype(jnp.bfloat16)
    where_ref[...] = slot_of


def best_kernel(got_ref, slot_ref, size_ref, best_ref, mean_ref, spread_ref):
    rows = got_ref.shape[0]
    depth = got_ref.shape[1] - LANES
    unit = got_ref[:, :depth]
    coded = got_ref[:, depth:]
    similar = lax.dot_general(
        unit, unit, (((1,), (1,)), ((), ())), preferred_element_type=jnp.float32
    )
    rank_col = coded.astype(jnp.float32)[:, :1]
    first = (iota((8, LANES), 1) == 0).astype(jnp.bfloat16)
    rank_row = lax.dot_general(
        first, coded, (((1,), (1,)), ((), ())), preferred_element_type=jnp.float32
    )[:1]
    same = ((iota((rows, rows), 0) ^ iota((rows, rows), 1)) & 1) == 0
    allowed = same & (rank_row > 0.0) & (rank_row < rank_col)
    best = jnp.max(jnp.where(allowed, similar, -1.0), axis=1, keepdims=True)
    spread_ref[...] = jnp.broadcast_to(best, spread_ref.shape)
    live_col = jnp.broadcast_to(rank_col, spread_ref.shape) > 0.0
    summed = jnp.where(live_col, spread_ref[...], 0.0)
    odd = (iota(spread_ref.shape, 0) & 1) == 1
    lane = iota((1, LANES), 1)
    total = jnp.where(
        lane == 0,
        jnp.sum(jnp.where(odd, 0.0, summed), axis=0, keepdims=True),
        jnp.sum(jnp.where(odd, summed, 0.0), axis=0, keepdims=True),
    )
    half = rows // 2
    even_best = spread_ref[pl.ds(0, half, stride=2), :]
    odd_best = spread_ref[pl.ds(1, half, stride=2), :]
    best_ref[...] = jnp.where(iota((half, LANES), 1) == 0, even_best, odd_best)
    first_slot = lax.axis_index("dev") * 2
    slots = slot_ref[...]
    sizes = size_ref[...]
    size0 = jnp.sum(jnp.where(slots == first_slot, sizes, 0), axis=1, keepdims=True)
    size1 = jnp.sum(jnp.where(slots == first_slot + 1, sizes, 0), axis=1, keepdims=True)
    size = jnp.where(lane == 0, size0, size1)
    mean_ref[...] = total / size.astype(jnp.float32)


def pick_kernel(back_ref, where_ref, best_ref, keep_ref):
    slot_of = where_ref[...]
    back = back_ref[...]
    owners = iota((back.shape[0], slot_of.shape[1]), 0)
    from_even = jnp.where(owners * 2 == slot_of, back[:, :1], 0.0)
    from_odd = jnp.where(owners * 2 + 1 == slot_of, back[:, 1:2], 0.0)
    best = jnp.sum(from_even + from_odd, axis=0, keepdims=True)
    best_ref[...] = best
    keep_ref[...] = (best < cutoff).astype(jnp.int32)


def body(embeddings, cluster_id, member_order, cluster_slot, cluster_size):
    devices = lax.axis_size("dev")
    rows, depth = embeddings.shape
    clusters = cluster_slot.shape[0]
    ids = cluster_id.reshape(1, rows)
    order = member_order.reshape(1, rows)
    slot = cluster_slot.reshape(1, clusters)
    size = cluster_size.reshape(1, clusters)
    width = depth + LANES
    payload, place = pl.pallas_call(
        place_kernel,
        out_shape=(
            jax.ShapeDtypeStruct((clusters, width), jnp.bfloat16),
            jax.ShapeDtypeStruct((1, rows), jnp.int32),
        ),
        name="place",
        compiler_params=pltpu.CompilerParams(vmem_limit_bytes=24 * 2**20),
    )(embeddings, ids, order, slot, size)
    got = lax.all_to_all(payload, "dev", split_axis=0, concat_axis=0, tiled=True)
    best, mean = pl.pallas_call(
        best_kernel,
        out_shape=(
            jax.ShapeDtypeStruct((devices, LANES), jnp.float32),
            jax.ShapeDtypeStruct((1, LANES), jnp.float32),
        ),
        scratch_shapes=[pltpu.VMEM((clusters, LANES), jnp.float32)],
        name="best",
        compiler_params=pltpu.CompilerParams(vmem_limit_bytes=24 * 2**20),
    )(got, slot, size)
    back = lax.all_to_all(
        best.reshape(devices, 1, LANES), "dev", split_axis=0, concat_axis=0, tiled=True
    ).reshape(devices, LANES)
    row_best, keep = pl.pallas_call(
        pick_kernel,
        out_shape=(
            jax.ShapeDtypeStruct((1, rows), jnp.float32),
            jax.ShapeDtypeStruct((1, rows), jnp.int32),
        ),
        name="pick",
        compiler_params=pltpu.CompilerParams(vmem_limit_bytes=24 * 2**20),
    )(back, place)
    return (row_best.reshape(rows), keep.reshape(rows), mean[0, :2])


def solution(mesh):
    placed = (P(("rep", "dev"), None), P(("rep", "dev")), P(("rep", "dev")), P("rep"), P("rep"))
    return jax.shard_map(
        body,
        mesh=mesh,
        in_specs=placed,
        out_specs=(P(("rep", "dev")), P(("rep", "dev")), P(("rep", "dev"))),
        check_vma=False,
    )
```

```python
import jax
import jax.numpy as jnp
from jax import lax
from jax.experimental import pallas as pl
from jax.experimental.pallas import tpu as pltpu
from jax.sharding import PartitionSpec as P

CAP = 128
LANES = 128
KERNEL_VMEM = 24 * 2**20

norm_eps = 1e-06
cutoff = 0.8


def iota(shape, axis):
    return lax.broadcasted_iota(jnp.int32, shape, axis)


def table_lookup(cluster_row, table_row):
    clusters = table_row.shape[1]
    hit = (iota((clusters, cluster_row.shape[1]), 0) == cluster_row).astype(jnp.bfloat16)
    table = jnp.broadcast_to(table_row.astype(jnp.bfloat16), (8, clusters))
    return jnp.dot(table, hit, preferred_element_type=jnp.float32)[:1]


def place_kernel(emb_ref, table_ref, out_ref, where_ref, own_ref):
    rows, depth = emb_ref.shape
    owners, tiles = out_ref.shape[0], depth // LANES
    clusters = 2 * owners
    ids = table_ref[:, :rows]
    order = table_ref[:, rows : 2 * rows]
    slots = table_ref[:, 2 * rows : 2 * rows + clusters]
    sizes = table_ref[:, 2 * rows + clusters :]
    slot_of = table_lookup(ids, slots).astype(jnp.int32)
    size_of = table_lookup(ids, sizes).astype(jnp.int32)
    where_ref[...] = slot_of
    code = jnp.where(order < size_of, order + 1, 0).astype(jnp.float32)
    hit = iota((clusters, rows), 0) == slot_of
    rank = jnp.sum(jnp.where(hit, code, 0.0), axis=1, keepdims=True)
    coded = jnp.broadcast_to(rank, (clusters, LANES)).astype(jnp.bfloat16)
    out_ref[:, tiles] = coded.reshape(owners, 2, LANES)
    first_slot = lax.axis_index("dev") * 2
    size0 = jnp.sum(jnp.where(slots == first_slot, sizes, 0), axis=1, keepdims=True)
    size1 = jnp.sum(jnp.where(slots == first_slot + 1, sizes, 0), axis=1, keepdims=True)
    own_ref[...] = jnp.where(iota((1, LANES), 1) == 0, size0, size1)
    values = emb_ref[...]
    squares_sum = jnp.sum(values * values, axis=1, keepdims=True)
    unit = (values * lax.rsqrt(squares_sum + norm_eps)).astype(jnp.bfloat16)
    pick = hit.astype(jnp.bfloat16)
    for c in range(0, tiles, 2):
        placed = jnp.dot(
            pick, unit[:, c * LANES : (c + 2) * LANES], preferred_element_type=jnp.float32
        ).astype(jnp.bfloat16)
        out_ref[:, c] = placed[:, :LANES].reshape(owners, 2, LANES)
        out_ref[:, c + 1] = placed[:, LANES:].reshape(owners, 2, LANES)


def best_kernel(got_ref, own_ref, best_ref, mean_ref, matrix, spread_ref):
    sources, tiles = got_ref.shape[:2]
    rows = 2 * sources
    for c in range(tiles):
        matrix[:, c * LANES : (c + 1) * LANES] = got_ref[:, c].reshape(rows, LANES)
    depth = (tiles - 1) * LANES
    unit = matrix[:, :depth]
    coded = matrix[:, depth:]
    similar = lax.dot_general(
        unit, unit, (((1,), (1,)), ((), ())), preferred_element_type=jnp.float32
    )
    rank_col = coded.astype(jnp.float32)[:, :1]
    first = (iota((8, LANES), 1) == 0).astype(jnp.bfloat16)
    rank_row = lax.dot_general(
        first, coded, (((1,), (1,)), ((), ())), preferred_element_type=jnp.float32
    )[:1]
    same = ((iota((rows, rows), 0) ^ iota((rows, rows), 1)) & 1) == 0
    allowed = same & (rank_row > 0.0) & (rank_row < rank_col)
    best = jnp.max(jnp.where(allowed, similar, -1.0), axis=1, keepdims=True)
    spread_ref[...] = jnp.broadcast_to(best, spread_ref.shape)
    live_col = jnp.broadcast_to(rank_col, spread_ref.shape) > 0.0
    summed = jnp.where(live_col, spread_ref[...], 0.0)
    odd = (iota(spread_ref.shape, 0) & 1) == 1
    lane = iota((1, LANES), 1)
    total = jnp.where(
        lane == 0,
        jnp.sum(jnp.where(odd, 0.0, summed), axis=0, keepdims=True),
        jnp.sum(jnp.where(odd, summed, 0.0), axis=0, keepdims=True),
    )
    even_best = spread_ref[pl.ds(0, sources, stride=2), :]
    odd_best = spread_ref[pl.ds(1, sources, stride=2), :]
    best_ref[...] = jnp.where(iota((sources, LANES), 1) == 0, even_best, odd_best)
    mean_ref[...] = total / own_ref[...].astype(jnp.float32)


def pick_kernel(back_ref, where_ref, best_ref, keep_ref):
    slot_of = where_ref[...]
    back = back_ref[...]
    owners = iota((back.shape[0], slot_of.shape[1]), 0)
    from_even = jnp.where(owners * 2 == slot_of, back[:, :1], 0.0)
    from_odd = jnp.where(owners * 2 + 1 == slot_of, back[:, 1:2], 0.0)
    best = jnp.sum(from_even + from_odd, axis=0, keepdims=True)
    best_ref[...] = best
    keep_ref[...] = (best < cutoff).astype(jnp.int32)


def body(embeddings, cluster_id, member_order, cluster_slot, cluster_size):
    devices = lax.axis_size("dev")
    rows, depth = embeddings.shape
    clusters = cluster_slot.shape[0]
    table = jnp.concatenate([cluster_id, member_order, cluster_slot, cluster_size])
    tiles = depth // LANES + 1
    payload, place, own = pl.pallas_call(
        place_kernel,
        out_shape=(
            jax.ShapeDtypeStruct((devices, tiles, 2, LANES), jnp.bfloat16),
            jax.ShapeDtypeStruct((1, rows), jnp.int32),
            jax.ShapeDtypeStruct((1, LANES), jnp.int32),
        ),
        name="place",
        compiler_params=pltpu.CompilerParams(vmem_limit_bytes=KERNEL_VMEM),
    )(embeddings, table.reshape(1, -1))
    got = lax.all_to_all(payload, "dev", split_axis=0, concat_axis=0, tiled=True)
    best, mean = pl.pallas_call(
        best_kernel,
        out_shape=(
            jax.ShapeDtypeStruct((devices, LANES), jnp.float32),
            jax.ShapeDtypeStruct((1, LANES), jnp.float32),
        ),
        scratch_shapes=[
            pltpu.VMEM((clusters, tiles * LANES), jnp.bfloat16),
            pltpu.VMEM((clusters, LANES), jnp.float32),
        ],
        name="best",
        compiler_params=pltpu.CompilerParams(vmem_limit_bytes=KERNEL_VMEM),
    )(got, own)
    back = lax.all_to_all(
        best.reshape(devices, 1, LANES), "dev", split_axis=0, concat_axis=0, tiled=True
    ).reshape(devices, LANES)
    row_best, keep = pl.pallas_call(
        pick_kernel,
        out_shape=(
            jax.ShapeDtypeStruct((1, rows), jnp.float32),
            jax.ShapeDtypeStruct((1, rows), jnp.int32),
        ),
        name="pick",
        compiler_params=pltpu.CompilerParams(vmem_limit_bytes=KERNEL_VMEM),
    )(back, place)
    return (row_best.reshape(rows), keep.reshape(rows), mean[0, :2])


def solution(mesh):
    placed = (P(("rep", "dev"), None), P(("rep", "dev")), P(("rep", "dev")), P("rep"), P("rep"))
    return jax.shard_map(
        body,
        mesh=mesh,
        in_specs=placed,
        out_specs=(P(("rep", "dev")), P(("rep", "dev")), P(("rep", "dev"))),
        check_vma=False,
    )
```

```python
import jax
import jax.numpy as jnp
from jax import lax
from jax.experimental import pallas as pl
from jax.experimental.pallas import tpu as pltpu
from jax.sharding import PartitionSpec as P

CAP = 128
LANES = 128
KERNEL_VMEM = 24 * 2**20
STEP = 8
IN_PARTS = 8
UNIT_VMEM = 52 * 2**20

norm_eps = 1e-06
cutoff = 0.8


def iota(shape, axis):
    return lax.broadcasted_iota(jnp.int32, shape, axis)


def table_lookup(cluster_row, table_row):
    clusters = table_row.shape[1]
    hit = (iota((clusters, cluster_row.shape[1]), 0) == cluster_row).astype(jnp.bfloat16)
    table = jnp.broadcast_to(table_row.astype(jnp.bfloat16), (8, clusters))
    return jnp.dot(table, hit, preferred_element_type=jnp.float32)[:1]


def unit_kernel(emb_ref, unit_ref, emb, sems):
    rows = emb.shape[0]
    part = rows // IN_PARTS
    copies = [
        pltpu.make_async_copy(
            emb_ref.at[pl.ds(k * part, part)], emb.at[pl.ds(k * part, part)], sems.at[k]
        )
        for k in range(IN_PARTS)
    ]
    for copy in copies:
        copy.start()
    for k, copy in enumerate(copies):
        copy.wait()
        values = emb[k * part : (k + 1) * part]
        squares_sum = jnp.sum(values * values, axis=1, keepdims=True)
        unit_ref[k * part : (k + 1) * part] = (
            values * lax.rsqrt(squares_sum + norm_eps)
        ).astype(jnp.bfloat16)


def place_kernel(unit_ref, id_ref, order_ref, slot_ref, size_ref, out_ref, where_ref, own_ref):
    rows, depth = unit_ref.shape
    owners, tiles = out_ref.shape[0], depth // LANES
    clusters = 2 * owners
    ids = id_ref[...]
    slots = slot_ref[...]
    sizes = size_ref[...]
    order = order_ref[...]
    slot_of = table_lookup(ids, slots).astype(jnp.int32)
    size_of = table_lookup(ids, sizes).astype(jnp.int32)
    where_ref[...] = slot_of
    code = jnp.where(order < size_of, order + 1, 0).astype(jnp.float32)
    hit = iota((clusters, rows), 0) == slot_of
    rank = jnp.sum(jnp.where(hit, code, 0.0), axis=1, keepdims=True)
    coded = jnp.broadcast_to(rank, (clusters, LANES)).astype(jnp.bfloat16)
    out_ref[:, tiles] = coded.reshape(owners, 2, LANES)
    first_slot = lax.axis_index("dev") * 2
    size0 = jnp.sum(jnp.where(slots == first_slot, sizes, 0), axis=1, keepdims=True)
    size1 = jnp.sum(jnp.where(slots == first_slot + 1, sizes, 0), axis=1, keepdims=True)
    own_ref[...] = jnp.where(iota((1, LANES), 1) == 0, size0, size1)
    pick = hit.astype(jnp.bfloat16)
    for c in range(0, tiles, 2):
        placed = jnp.dot(
            pick, unit_ref[:, c * LANES : (c + 2) * LANES], preferred_element_type=jnp.float32
        ).astype(jnp.bfloat16)
        out_ref[:, c] = placed[:, :LANES].reshape(owners, 2, LANES)
        out_ref[:, c + 1] = placed[:, LANES:].reshape(owners, 2, LANES)


def best_kernel(got_ref, own_ref, best_ref, mean_ref, spread_ref):
    sources, tiles = got_ref.shape[0], got_ref.shape[1] - 1
    rows = 2 * sources
    similar = jnp.zeros((rows, rows), jnp.float32)
    for q in range(0, tiles, STEP):
        unit = jnp.concatenate(
            [got_ref[:, c].reshape(rows, LANES) for c in range(q, q + STEP)], axis=1
        )
        similar += lax.dot_general(
            unit, unit, (((1,), (1,)), ((), ())), preferred_element_type=jnp.float32
        )
    coded = got_ref[:, tiles].reshape(rows, LANES)
    rank_col = coded.astype(jnp.float32)[:, :1]
    first = (iota((8, LANES), 1) == 0).astype(jnp.bfloat16)
    rank_row = lax.dot_general(
        first, coded, (((1,), (1,)), ((), ())), preferred_element_type=jnp.float32
    )[:1]
    same = ((iota((rows, rows), 0) ^ iota((rows, rows), 1)) & 1) == 0
    allowed = same & (rank_row > 0.0) & (rank_row < rank_col)
    best = jnp.max(jnp.where(allowed, similar, -1.0), axis=1, keepdims=True)
    spread_ref[...] = jnp.broadcast_to(best, spread_ref.shape)
    live_col = jnp.broadcast_to(rank_col, spread_ref.shape) > 0.0
    summed = jnp.where(live_col, spread_ref[...], 0.0)
    odd = (iota(spread_ref.shape, 0) & 1) == 1
    lane = iota((1, LANES), 1)
    total = jnp.where(
        lane == 0,
        jnp.sum(jnp.where(odd, 0.0, summed), axis=0, keepdims=True),
        jnp.sum(jnp.where(odd, summed, 0.0), axis=0, keepdims=True),
    )
    even_best = spread_ref[pl.ds(0, sources, stride=2), :]
    odd_best = spread_ref[pl.ds(1, sources, stride=2), :]
    best_ref[...] = jnp.where(iota((sources, LANES), 1) == 0, even_best, odd_best)
    mean_ref[...] = total / own_ref[...].astype(jnp.float32)


def pick_kernel(back_ref, where_ref, best_ref, keep_ref):
    slot_of = where_ref[...]
    back = back_ref[...]
    owners = iota((back.shape[0], slot_of.shape[1]), 0)
    from_even = jnp.where(owners * 2 == slot_of, back[:, :1], 0.0)
    from_odd = jnp.where(owners * 2 + 1 == slot_of, back[:, 1:2], 0.0)
    best = jnp.sum(from_even + from_odd, axis=0, keepdims=True)
    best_ref[...] = best
    keep_ref[...] = (best < cutoff).astype(jnp.int32)


def body(embeddings, cluster_id, member_order, cluster_slot, cluster_size):
    devices = lax.axis_size("dev")
    rows, depth = embeddings.shape
    clusters = cluster_slot.shape[0]
    tiles = depth // LANES + 1
    unit = pl.pallas_call(
        unit_kernel,
        out_shape=jax.ShapeDtypeStruct((rows, depth), jnp.bfloat16),
        in_specs=[pl.BlockSpec(memory_space=pltpu.HBM)],
        scratch_shapes=[
            pltpu.VMEM((rows, depth), jnp.float32),
            pltpu.SemaphoreType.DMA((IN_PARTS,)),
        ],
        name="unit",
        compiler_params=pltpu.CompilerParams(vmem_limit_bytes=UNIT_VMEM),
    )(embeddings)
    payload, place, own = pl.pallas_call(
        place_kernel,
        out_shape=(
            jax.ShapeDtypeStruct((devices, tiles, 2, LANES), jnp.bfloat16),
            jax.ShapeDtypeStruct((1, rows), jnp.int32),
            jax.ShapeDtypeStruct((1, LANES), jnp.int32),
        ),
        name="place",
        compiler_params=pltpu.CompilerParams(vmem_limit_bytes=KERNEL_VMEM),
    )(
        unit,
        cluster_id.reshape(1, rows),
        member_order.reshape(1, rows),
        cluster_slot.reshape(1, clusters),
        cluster_size.reshape(1, clusters),
    )
    got = lax.all_to_all(payload, "dev", split_axis=0, concat_axis=0, tiled=True)
    best, mean = pl.pallas_call(
        best_kernel,
        out_shape=(
            jax.ShapeDtypeStruct((devices, LANES), jnp.float32),
            jax.ShapeDtypeStruct((1, LANES), jnp.float32),
        ),
        scratch_shapes=[
            pltpu.VMEM((clusters, LANES), jnp.float32),
        ],
        name="best",
        compiler_params=pltpu.CompilerParams(vmem_limit_bytes=KERNEL_VMEM),
    )(got, own)
    back = lax.all_to_all(
        best.reshape(devices, 1, LANES), "dev", split_axis=0, concat_axis=0, tiled=True
    ).reshape(devices, LANES)
    row_best, keep = pl.pallas_call(
        pick_kernel,
        out_shape=(
            jax.ShapeDtypeStruct((1, rows), jnp.float32),
            jax.ShapeDtypeStruct((1, rows), jnp.int32),
        ),
        name="pick",
        compiler_params=pltpu.CompilerParams(vmem_limit_bytes=KERNEL_VMEM),
    )(back, place)
    return (row_best.reshape(rows), keep.reshape(rows), mean[0, :2])


def solution(mesh):
    placed = (P(("rep", "dev"), None), P(("rep", "dev")), P(("rep", "dev")), P("rep"), P("rep"))
    return jax.shard_map(
        body,
        mesh=mesh,
        in_specs=placed,
        out_specs=(P(("rep", "dev")), P(("rep", "dev")), P(("rep", "dev"))),
        check_vma=False,
    )
```

```python
import jax
import jax.numpy as jnp
from jax import lax
from jax.experimental import pallas as pl
from jax.experimental.pallas import tpu as pltpu
from jax.sharding import PartitionSpec as P

CAP = 128
LANES = 128
KERNEL_VMEM = 24 * 2**20
STEP = 8
IN_PARTS = 8
UNIT_VMEM = 52 * 2**20

norm_eps = 1e-06
cutoff = 0.8


def iota(shape, axis):
    return lax.broadcasted_iota(jnp.int32, shape, axis)


def table_lookup(cluster_row, table_row):
    clusters = table_row.shape[1]
    hit = (iota((clusters, cluster_row.shape[1]), 0) == cluster_row).astype(jnp.bfloat16)
    table = jnp.broadcast_to(table_row.astype(jnp.bfloat16), (8, clusters))
    return jnp.dot(table, hit, preferred_element_type=jnp.float32)[:1]


def unit_kernel(emb_ref, unit_ref, emb, sems):
    rows = emb.shape[0]
    part = rows // IN_PARTS
    copies = [
        pltpu.make_async_copy(
            emb_ref.at[pl.ds(k * part, part)], emb.at[pl.ds(k * part, part)], sems.at[k]
        )
        for k in range(IN_PARTS)
    ]
    for copy in copies:
        copy.start()
    for k, copy in enumerate(copies):
        copy.wait()
        values = emb[k * part : (k + 1) * part]
        squares_sum = jnp.sum(values * values, axis=1, keepdims=True)
        unit_ref[k * part : (k + 1) * part] = (
            values * lax.rsqrt(squares_sum + norm_eps)
        ).astype(jnp.bfloat16)


def place_kernel(unit_ref, id_ref, order_ref, slot_ref, size_ref, out_ref, where_ref, own_ref):
    rows, depth = unit_ref.shape
    owners, tiles = out_ref.shape[0], depth // LANES
    clusters = 2 * owners
    ids = id_ref[...]
    slots = slot_ref[...]
    sizes = size_ref[...]
    order = order_ref[...]
    slot_of = table_lookup(ids, slots).astype(jnp.int32)
    size_of = table_lookup(ids, sizes).astype(jnp.int32)
    where_ref[...] = slot_of
    code = jnp.where(order < size_of, order + 1, 0).astype(jnp.float32)
    hit = iota((clusters, rows), 0) == slot_of
    rank = jnp.sum(jnp.where(hit, code, 0.0), axis=1, keepdims=True)
    coded = jnp.broadcast_to(rank, (clusters, LANES)).astype(jnp.bfloat16)
    out_ref[:, tiles] = coded.reshape(owners, 2, LANES)
    first_slot = lax.axis_index("dev") * 2
    size0 = jnp.sum(jnp.where(slots == first_slot, sizes, 0), axis=1, keepdims=True)
    size1 = jnp.sum(jnp.where(slots == first_slot + 1, sizes, 0), axis=1, keepdims=True)
    own_ref[...] = jnp.where(iota((1, LANES), 1) == 0, size0, size1)
    pick = hit.astype(jnp.bfloat16)
    for c in range(0, tiles, 2):
        placed = jnp.dot(
            pick, unit_ref[:, c * LANES : (c + 2) * LANES], preferred_element_type=jnp.float32
        ).astype(jnp.bfloat16)
        out_ref[:, c] = placed[:, :LANES].reshape(owners, 2, LANES)
        out_ref[:, c + 1] = placed[:, LANES:].reshape(owners, 2, LANES)


def best_kernel(got_ref, own_ref, best_ref, mean_ref, spread_ref):
    sources, tiles = got_ref.shape[0], got_ref.shape[1] - 1
    rows = 2 * sources
    similar = jnp.zeros((rows, rows), jnp.float32)
    for q in range(0, tiles, STEP):
        unit = jnp.concatenate(
            [got_ref[:, c].reshape(rows, LANES) for c in range(q, q + STEP)], axis=1
        )
        similar += lax.dot_general(
            unit, unit, (((1,), (1,)), ((), ())), preferred_element_type=jnp.float32
        )
    coded = got_ref[:, tiles].reshape(rows, LANES)
    rank_col = coded.astype(jnp.float32)[:, :1]
    first = (iota((8, LANES), 1) == 0).astype(jnp.bfloat16)
    rank_row = lax.dot_general(
        first, coded, (((1,), (1,)), ((), ())), preferred_element_type=jnp.float32
    )[:1]
    same = ((iota((rows, rows), 0) ^ iota((rows, rows), 1)) & 1) == 0
    allowed = same & (rank_row > 0.0) & (rank_row < rank_col)
    best = jnp.max(jnp.where(allowed, similar, -1.0), axis=1, keepdims=True)
    spread_ref[...] = jnp.broadcast_to(best, spread_ref.shape)
    live_col = jnp.broadcast_to(rank_col, spread_ref.shape) > 0.0
    summed = jnp.where(live_col, spread_ref[...], 0.0)
    odd = (iota(spread_ref.shape, 0) & 1) == 1
    lane = iota((1, LANES), 1)
    total = jnp.where(
        lane == 0,
        jnp.sum(jnp.where(odd, 0.0, summed), axis=0, keepdims=True),
        jnp.sum(jnp.where(odd, summed, 0.0), axis=0, keepdims=True),
    )
    even_best = spread_ref[pl.ds(0, sources, stride=2), :]
    odd_best = spread_ref[pl.ds(1, sources, stride=2), :]
    best_ref[...] = jnp.where(iota((sources, LANES), 1) == 0, even_best, odd_best)
    mean_ref[...] = (total / own_ref[...].astype(jnp.float32))[:, : mean_ref.shape[1]]


def pick_kernel(back_ref, where_ref, best_ref, keep_ref):
    slot_of = where_ref[...]
    back = back_ref[...]
    owners = iota((back.shape[0], slot_of.shape[1]), 0)
    from_even = jnp.where(owners * 2 == slot_of, back[:, :1], 0.0)
    from_odd = jnp.where(owners * 2 + 1 == slot_of, back[:, 1:2], 0.0)
    best = jnp.sum(from_even + from_odd, axis=0, keepdims=True)
    best_ref[...] = best
    keep_ref[...] = (best < cutoff).astype(jnp.int32)


def body(embeddings, cluster_id, member_order, cluster_slot, cluster_size):
    devices = lax.axis_size("dev")
    rows, depth = embeddings.shape
    clusters = cluster_slot.shape[0]
    tiles = depth // LANES + 1
    unit = pl.pallas_call(
        unit_kernel,
        out_shape=jax.ShapeDtypeStruct((rows, depth), jnp.bfloat16),
        in_specs=[pl.BlockSpec(memory_space=pltpu.HBM)],
        scratch_shapes=[
            pltpu.VMEM((rows, depth), jnp.float32),
            pltpu.SemaphoreType.DMA((IN_PARTS,)),
        ],
        name="unit",
        compiler_params=pltpu.CompilerParams(vmem_limit_bytes=UNIT_VMEM),
    )(embeddings)
    payload, place, own = pl.pallas_call(
        place_kernel,
        out_shape=(
            jax.ShapeDtypeStruct((devices, tiles, 2, LANES), jnp.bfloat16),
            jax.ShapeDtypeStruct((1, rows), jnp.int32),
            jax.ShapeDtypeStruct((1, LANES), jnp.int32),
        ),
        name="place",
        compiler_params=pltpu.CompilerParams(vmem_limit_bytes=KERNEL_VMEM),
    )(
        unit,
        cluster_id.reshape(1, rows),
        member_order.reshape(1, rows),
        cluster_slot.reshape(1, clusters),
        cluster_size.reshape(1, clusters),
    )
    got = lax.all_to_all(payload, "dev", split_axis=0, concat_axis=0, tiled=True)
    best, mean = pl.pallas_call(
        best_kernel,
        out_shape=(
            jax.ShapeDtypeStruct((devices, LANES), jnp.float32),
            jax.ShapeDtypeStruct((1, 2), jnp.float32),
        ),
        scratch_shapes=[
            pltpu.VMEM((clusters, LANES), jnp.float32),
        ],
        name="best",
        compiler_params=pltpu.CompilerParams(vmem_limit_bytes=KERNEL_VMEM),
    )(got, own)
    back = lax.all_to_all(
        best.reshape(devices, 1, LANES), "dev", split_axis=0, concat_axis=0, tiled=True
    ).reshape(devices, LANES)
    row_best, keep = pl.pallas_call(
        pick_kernel,
        out_shape=(
            jax.ShapeDtypeStruct((1, rows), jnp.float32),
            jax.ShapeDtypeStruct((1, rows), jnp.int32),
        ),
        name="pick",
        compiler_params=pltpu.CompilerParams(vmem_limit_bytes=KERNEL_VMEM),
    )(back, place)
    return (row_best.reshape(rows), keep.reshape(rows), mean.reshape(2))


def solution(mesh):
    placed = (P(("rep", "dev"), None), P(("rep", "dev")), P(("rep", "dev")), P("rep"), P("rep"))
    return jax.shard_map(
        body,
        mesh=mesh,
        in_specs=placed,
        out_specs=(P(("rep", "dev")), P(("rep", "dev")), P(("rep", "dev"))),
        check_vma=False,
    )
```

```python
import jax
import jax.numpy as jnp
from jax import lax
from jax.experimental import pallas as pl
from jax.experimental.pallas import tpu as pltpu
from jax.sharding import PartitionSpec as P

CAP = 128
LANES = 128
KERNEL_VMEM = 24 * 2**20
STEP = 8
IN_PARTS = 8

norm_eps = 1e-06
cutoff = 0.8


def iota(shape, axis):
    return lax.broadcasted_iota(jnp.int32, shape, axis)


def table_lookup(cluster_row, table_row):
    clusters = table_row.shape[1]
    hit = (iota((clusters, cluster_row.shape[1]), 0) == cluster_row).astype(jnp.bfloat16)
    table = jnp.broadcast_to(table_row.astype(jnp.bfloat16), (8, clusters))
    return jnp.dot(table, hit, preferred_element_type=jnp.float32)[:1]


def place_kernel(
    emb_ref, id_ref, order_ref, slot_ref, size_ref,
    out_ref, where_ref, own_ref,
    emb, unit, ids_v, order_v, slot_v, size_v, sems,
):
    rows, depth = emb.shape
    part = rows // IN_PARTS
    owners, tiles = out_ref.shape[0], depth // LANES
    clusters = 2 * owners
    small = [
        pltpu.make_async_copy(source, target, sems.at[k])
        for k, (source, target) in enumerate(
            ((id_ref, ids_v), (slot_ref, slot_v), (order_ref, order_v), (size_ref, size_v))
        )
    ]
    large = [
        pltpu.make_async_copy(
            emb_ref.at[pl.ds(k * part, part)], emb.at[pl.ds(k * part, part)], sems.at[4 + k]
        )
        for k in range(IN_PARTS)
    ]
    for copy in small + large:
        copy.start()
    for copy in small:
        copy.wait()
    ids = ids_v[...]
    order = order_v[...]
    slots = slot_v[...]
    sizes = size_v[...]
    slot_of = table_lookup(ids, slots).astype(jnp.int32)
    size_of = table_lookup(ids, sizes).astype(jnp.int32)
    where_ref[...] = slot_of
    code = jnp.where(order < size_of, order + 1, 0).astype(jnp.float32)
    hit = iota((clusters, rows), 0) == slot_of
    rank = jnp.sum(jnp.where(hit, code, 0.0), axis=1, keepdims=True)
    coded = jnp.broadcast_to(rank, (clusters, LANES)).astype(jnp.bfloat16)
    out_ref[:, tiles] = coded.reshape(owners, 2, LANES)
    first_slot = lax.axis_index("dev") * 2
    size0 = jnp.sum(jnp.where(slots == first_slot, sizes, 0), axis=1, keepdims=True)
    size1 = jnp.sum(jnp.where(slots == first_slot + 1, sizes, 0), axis=1, keepdims=True)
    own_ref[...] = jnp.where(iota((1, LANES), 1) == 0, size0, size1)
    pick = hit.astype(jnp.bfloat16)
    for k, copy in enumerate(large):
        copy.wait()
        values = emb[k * part : (k + 1) * part]
        squares_sum = jnp.sum(values * values, axis=1, keepdims=True)
        unit[k * part : (k + 1) * part] = (
            values * lax.rsqrt(squares_sum + norm_eps)
        ).astype(jnp.bfloat16)
    for c in range(0, tiles, 2):
        placed = jnp.dot(
            pick, unit[:, c * LANES : (c + 2) * LANES], preferred_element_type=jnp.float32
        ).astype(jnp.bfloat16)
        out_ref[:, c] = placed[:, :LANES].reshape(owners, 2, LANES)
        out_ref[:, c + 1] = placed[:, LANES:].reshape(owners, 2, LANES)


def best_kernel(got_ref, own_ref, best_ref, mean_ref, spread_ref):
    sources, tiles = got_ref.shape[0], got_ref.shape[1] - 1
    rows = 2 * sources
    similar = jnp.zeros((rows, rows), jnp.float32)
    for q in range(0, tiles, STEP):
        unit = jnp.concatenate(
            [got_ref[:, c].reshape(rows, LANES) for c in range(q, q + STEP)], axis=1
        )
        similar += lax.dot_general(
            unit, unit, (((1,), (1,)), ((), ())), preferred_element_type=jnp.float32
        )
    coded = got_ref[:, tiles].reshape(rows, LANES)
    rank_col = coded.astype(jnp.float32)[:, :1]
    first = (iota((8, LANES), 1) == 0).astype(jnp.bfloat16)
    rank_row = lax.dot_general(
        first, coded, (((1,), (1,)), ((), ())), preferred_element_type=jnp.float32
    )[:1]
    same = ((iota((rows, rows), 0) ^ iota((rows, rows), 1)) & 1) == 0
    allowed = same & (rank_row > 0.0) & (rank_row < rank_col)
    best = jnp.max(jnp.where(allowed, similar, -1.0), axis=1, keepdims=True)
    spread_ref[...] = jnp.broadcast_to(best, spread_ref.shape)
    live_col = jnp.broadcast_to(rank_col, spread_ref.shape) > 0.0
    summed = jnp.where(live_col, spread_ref[...], 0.0)
    odd = (iota(spread_ref.shape, 0) & 1) == 1
    lane = iota((1, LANES), 1)
    total = jnp.where(
        lane == 0,
        jnp.sum(jnp.where(odd, 0.0, summed), axis=0, keepdims=True),
        jnp.sum(jnp.where(odd, summed, 0.0), axis=0, keepdims=True),
    )
    even_best = spread_ref[pl.ds(0, sources, stride=2), :]
    odd_best = spread_ref[pl.ds(1, sources, stride=2), :]
    best_ref[...] = jnp.where(iota((sources, LANES), 1) == 0, even_best, odd_best)
    mean_ref[...] = (total / own_ref[...].astype(jnp.float32))[:, : mean_ref.shape[1]]


def pick_kernel(back_ref, where_ref, best_ref, keep_ref):
    slot_of = where_ref[...]
    back = back_ref[...]
    owners = iota((back.shape[0], slot_of.shape[1]), 0)
    from_even = jnp.where(owners * 2 == slot_of, back[:, :1], 0.0)
    from_odd = jnp.where(owners * 2 + 1 == slot_of, back[:, 1:2], 0.0)
    best = jnp.sum(from_even + from_odd, axis=0, keepdims=True)
    best_ref[...] = best
    keep_ref[...] = (best < cutoff).astype(jnp.int32)


def body(embeddings, cluster_id, member_order, cluster_slot, cluster_size):
    devices = lax.axis_size("dev")
    rows, depth = embeddings.shape
    clusters = cluster_slot.shape[0]
    tiles = depth // LANES + 1
    sources = (
        embeddings,
        cluster_id.reshape(1, rows),
        member_order.reshape(1, rows),
        cluster_slot.reshape(1, clusters),
        cluster_size.reshape(1, clusters),
    )
    payload, place, own = pl.pallas_call(
        place_kernel,
        out_shape=(
            jax.ShapeDtypeStruct((devices, tiles, 2, LANES), jnp.bfloat16),
            jax.ShapeDtypeStruct((1, rows), jnp.int32),
            jax.ShapeDtypeStruct((1, LANES), jnp.int32),
        ),
        in_specs=[pl.BlockSpec(memory_space=pltpu.HBM)] * len(sources),
        scratch_shapes=[
            pltpu.VMEM((rows, depth), jnp.float32),
            pltpu.VMEM((rows, depth), jnp.bfloat16),
            pltpu.VMEM((1, rows), jnp.int32),
            pltpu.VMEM((1, rows), jnp.int32),
            pltpu.VMEM((1, clusters), jnp.int32),
            pltpu.VMEM((1, clusters), jnp.int32),
            pltpu.SemaphoreType.DMA((4 + IN_PARTS,)),
        ],
        name="place",
        compiler_params=pltpu.CompilerParams(vmem_limit_bytes=KERNEL_VMEM),
    )(*[pltpu.with_memory_space_constraint(x, pltpu.HBM) for x in sources])
    got = lax.all_to_all(payload, "dev", split_axis=0, concat_axis=0, tiled=True)
    best, mean = pl.pallas_call(
        best_kernel,
        out_shape=(
            jax.ShapeDtypeStruct((devices, LANES), jnp.float32),
            jax.ShapeDtypeStruct((1, 2), jnp.float32),
        ),
        scratch_shapes=[
            pltpu.VMEM((clusters, LANES), jnp.float32),
        ],
        name="best",
        compiler_params=pltpu.CompilerParams(vmem_limit_bytes=KERNEL_VMEM),
    )(got, own)
    back = lax.all_to_all(
        best.reshape(devices, 1, LANES), "dev", split_axis=0, concat_axis=0, tiled=True
    ).reshape(devices, LANES)
    row_best, keep = pl.pallas_call(
        pick_kernel,
        out_shape=(
            jax.ShapeDtypeStruct((1, rows), jnp.float32),
            jax.ShapeDtypeStruct((1, rows), jnp.int32),
        ),
        name="pick",
        compiler_params=pltpu.CompilerParams(vmem_limit_bytes=KERNEL_VMEM),
    )(back, place)
    return (row_best.reshape(rows), keep.reshape(rows), mean.reshape(2))


def solution(mesh):
    placed = (P(("rep", "dev"), None), P(("rep", "dev")), P(("rep", "dev")), P("rep"), P("rep"))
    return jax.shard_map(
        body,
        mesh=mesh,
        in_specs=placed,
        out_specs=(P(("rep", "dev")), P(("rep", "dev")), P(("rep", "dev"))),
        check_vma=False,
    )
```

```python
import jax
import jax.numpy as jnp
from jax import lax
from jax.experimental import pallas as pl
from jax.experimental.pallas import tpu as pltpu
from jax.sharding import PartitionSpec as P

CAP = 128
LANES = 128
KERNEL_VMEM = 24 * 2**20
STEP = 8
IN_PARTS = 8

norm_eps = 1e-06
cutoff = 0.8


def iota(shape, axis):
    return lax.broadcasted_iota(jnp.int32, shape, axis)


def table_lookup(cluster_row, table_row):
    clusters = table_row.shape[1]
    hit = (iota((clusters, cluster_row.shape[1]), 0) == cluster_row).astype(jnp.bfloat16)
    table = jnp.broadcast_to(table_row.astype(jnp.bfloat16), (8, clusters))
    return jnp.dot(table, hit, preferred_element_type=jnp.float32)[:1]


def chunk_of(device, devices):
    return devices - 1 - device


def chunk_slot(slot, devices):
    return chunk_of(slot >> 1, devices) * 2 + (slot & 1)


def exchange(x, devices):
    order = sorted(range(devices), key=lambda device: chunk_of(device, devices))
    return lax.all_to_all(
        x, "dev", split_axis=0, concat_axis=0, axis_index_groups=[order], tiled=True
    )


def place_kernel(
    emb_ref, id_ref, order_ref, slot_ref, size_ref,
    out_ref, where_ref, own_ref,
    emb, unit, ids_v, order_v, slot_v, size_v, sems,
):
    rows, depth = emb.shape
    part = rows // IN_PARTS
    owners, tiles = out_ref.shape[0], depth // LANES
    clusters = 2 * owners
    small = [
        pltpu.make_async_copy(source, target, sems.at[k])
        for k, (source, target) in enumerate(
            ((id_ref, ids_v), (slot_ref, slot_v), (order_ref, order_v), (size_ref, size_v))
        )
    ]
    large = [
        pltpu.make_async_copy(
            emb_ref.at[pl.ds(k * part, part)], emb.at[pl.ds(k * part, part)], sems.at[4 + k]
        )
        for k in range(IN_PARTS)
    ]
    for copy in small + large:
        copy.start()
    for copy in small:
        copy.wait()
    ids = ids_v[...]
    order = order_v[...]
    slots = slot_v[...]
    sizes = size_v[...]
    slot_of = chunk_slot(table_lookup(ids, slots).astype(jnp.int32), owners)
    size_of = table_lookup(ids, sizes).astype(jnp.int32)
    where_ref[...] = slot_of
    code = jnp.where(order < size_of, order + 1, 0).astype(jnp.float32)
    hit = iota((clusters, rows), 0) == slot_of
    rank = jnp.sum(jnp.where(hit, code, 0.0), axis=1, keepdims=True)
    coded = jnp.broadcast_to(rank, (clusters, LANES)).astype(jnp.bfloat16)
    out_ref[:, tiles] = coded.reshape(owners, 2, LANES)
    first_slot = lax.axis_index("dev") * 2
    size0 = jnp.sum(jnp.where(slots == first_slot, sizes, 0), axis=1, keepdims=True)
    size1 = jnp.sum(jnp.where(slots == first_slot + 1, sizes, 0), axis=1, keepdims=True)
    own_ref[...] = jnp.where(iota((1, LANES), 1) == 0, size0, size1)
    pick = hit.astype(jnp.bfloat16)
    for k, copy in enumerate(large):
        copy.wait()
        values = emb[k * part : (k + 1) * part]
        squares_sum = jnp.sum(values * values, axis=1, keepdims=True)
        unit[k * part : (k + 1) * part] = (
            values * lax.rsqrt(squares_sum + norm_eps)
        ).astype(jnp.bfloat16)
    for c in range(0, tiles, 2):
        placed = jnp.dot(
            pick, unit[:, c * LANES : (c + 2) * LANES], preferred_element_type=jnp.float32
        ).astype(jnp.bfloat16)
        out_ref[:, c] = placed[:, :LANES].reshape(owners, 2, LANES)
        out_ref[:, c + 1] = placed[:, LANES:].reshape(owners, 2, LANES)


def best_kernel(got_ref, own_ref, best_ref, mean_ref, spread_ref):
    sources, tiles = got_ref.shape[0], got_ref.shape[1] - 1
    rows = 2 * sources
    similar = jnp.zeros((rows, rows), jnp.float32)
    for q in range(0, tiles, STEP):
        unit = jnp.concatenate(
            [got_ref[:, c].reshape(rows, LANES) for c in range(q, q + STEP)], axis=1
        )
        similar += lax.dot_general(
            unit, unit, (((1,), (1,)), ((), ())), preferred_element_type=jnp.float32
        )
    coded = got_ref[:, tiles].reshape(rows, LANES)
    rank_col = coded.astype(jnp.float32)[:, :1]
    first = (iota((8, LANES), 1) == 0).astype(jnp.bfloat16)
    rank_row = lax.dot_general(
        first, coded, (((1,), (1,)), ((), ())), preferred_element_type=jnp.float32
    )[:1]
    same = ((iota((rows, rows), 0) ^ iota((rows, rows), 1)) & 1) == 0
    allowed = same & (rank_row > 0.0) & (rank_row < rank_col)
    best = jnp.max(jnp.where(allowed, similar, -1.0), axis=1, keepdims=True)
    spread_ref[...] = jnp.broadcast_to(best, spread_ref.shape)
    live_col = jnp.broadcast_to(rank_col, spread_ref.shape) > 0.0
    summed = jnp.where(live_col, spread_ref[...], 0.0)
    odd = (iota(spread_ref.shape, 0) & 1) == 1
    lane = iota((1, LANES), 1)
    total = jnp.where(
        lane == 0,
        jnp.sum(jnp.where(odd, 0.0, summed), axis=0, keepdims=True),
        jnp.sum(jnp.where(odd, summed, 0.0), axis=0, keepdims=True),
    )
    even_best = spread_ref[pl.ds(0, sources, stride=2), :]
    odd_best = spread_ref[pl.ds(1, sources, stride=2), :]
    best_ref[...] = jnp.where(iota((sources, LANES), 1) == 0, even_best, odd_best)
    mean_ref[...] = (total / own_ref[...].astype(jnp.float32))[:, : mean_ref.shape[1]]


def pick_kernel(back_ref, where_ref, best_ref, keep_ref):
    slot_of = where_ref[...]
    back = back_ref[...]
    owners = iota((back.shape[0], slot_of.shape[1]), 0)
    from_even = jnp.where(owners * 2 == slot_of, back[:, :1], 0.0)
    from_odd = jnp.where(owners * 2 + 1 == slot_of, back[:, 1:2], 0.0)
    best = jnp.sum(from_even + from_odd, axis=0, keepdims=True)
    best_ref[...] = best
    keep_ref[...] = (best < cutoff).astype(jnp.int32)


def body(embeddings, cluster_id, member_order, cluster_slot, cluster_size):
    devices = lax.axis_size("dev")
    rows, depth = embeddings.shape
    clusters = cluster_slot.shape[0]
    tiles = depth // LANES + 1
    sources = (
        embeddings,
        cluster_id.reshape(1, rows),
        member_order.reshape(1, rows),
        cluster_slot.reshape(1, clusters),
        cluster_size.reshape(1, clusters),
    )
    payload, place, own = pl.pallas_call(
        place_kernel,
        out_shape=(
            jax.ShapeDtypeStruct((devices, tiles, 2, LANES), jnp.bfloat16),
            jax.ShapeDtypeStruct((1, rows), jnp.int32),
            jax.ShapeDtypeStruct((1, LANES), jnp.int32),
        ),
        in_specs=[pl.BlockSpec(memory_space=pltpu.HBM)] * len(sources),
        scratch_shapes=[
            pltpu.VMEM((rows, depth), jnp.float32),
            pltpu.VMEM((rows, depth), jnp.bfloat16),
            pltpu.VMEM((1, rows), jnp.int32),
            pltpu.VMEM((1, rows), jnp.int32),
            pltpu.VMEM((1, clusters), jnp.int32),
            pltpu.VMEM((1, clusters), jnp.int32),
            pltpu.SemaphoreType.DMA((4 + IN_PARTS,)),
        ],
        name="place",
        compiler_params=pltpu.CompilerParams(vmem_limit_bytes=KERNEL_VMEM),
    )(*[pltpu.with_memory_space_constraint(x, pltpu.HBM) for x in sources])
    got = exchange(payload, devices)
    best, mean = pl.pallas_call(
        best_kernel,
        out_shape=(
            jax.ShapeDtypeStruct((devices, LANES), jnp.float32),
            jax.ShapeDtypeStruct((1, 2), jnp.float32),
        ),
        scratch_shapes=[
            pltpu.VMEM((clusters, LANES), jnp.float32),
        ],
        name="best",
        compiler_params=pltpu.CompilerParams(vmem_limit_bytes=KERNEL_VMEM),
    )(got, own)
    back = exchange(best.reshape(devices, 1, LANES), devices).reshape(devices, LANES)
    row_best, keep = pl.pallas_call(
        pick_kernel,
        out_shape=(
            jax.ShapeDtypeStruct((1, rows), jnp.float32),
            jax.ShapeDtypeStruct((1, rows), jnp.int32),
        ),
        name="pick",
        compiler_params=pltpu.CompilerParams(vmem_limit_bytes=KERNEL_VMEM),
    )(back, place)
    return (row_best.reshape(rows), keep.reshape(rows), mean.reshape(2))


def solution(mesh):
    placed = (P(("rep", "dev"), None), P(("rep", "dev")), P(("rep", "dev")), P("rep"), P("rep"))
    return jax.shard_map(
        body,
        mesh=mesh,
        in_specs=placed,
        out_specs=(P(("rep", "dev")), P(("rep", "dev")), P(("rep", "dev"))),
        check_vma=False,
    )
```

```python
import jax
import jax.numpy as jnp
from jax import lax
from jax.experimental import pallas as pl
from jax.experimental.pallas import tpu as pltpu
from jax.sharding import PartitionSpec as P

CAP = 128
LANES = 128
KERNEL_VMEM = 24 * 2**20
STEP = 8
IN_PARTS = 8

norm_eps = 1e-06
cutoff = 0.8


def iota(shape, axis):
    return lax.broadcasted_iota(jnp.int32, shape, axis)


def table_lookup(cluster_row, table_row):
    clusters = table_row.shape[1]
    hit = (iota((clusters, cluster_row.shape[1]), 0) == cluster_row).astype(jnp.bfloat16)
    table = jnp.broadcast_to(table_row.astype(jnp.bfloat16), (8, clusters))
    return jnp.dot(table, hit, preferred_element_type=jnp.float32)[:1]


def chunk_of(device, devices):
    y, x, z = device >> 5, (device >> 3) & 3, device & 7
    return devices - 1 - ((((y + 1) & 3) << 5) | (((x + 1) & 3) << 3) | ((z * 3) & 7))


def chunk_slot(slot, devices):
    return chunk_of(slot >> 1, devices) * 2 + (slot & 1)


def exchange(x, devices):
    order = sorted(range(devices), key=lambda device: chunk_of(device, devices))
    return lax.all_to_all(
        x, "dev", split_axis=0, concat_axis=0, axis_index_groups=[order], tiled=True
    )


def place_kernel(
    emb_ref, id_ref, order_ref, slot_ref, size_ref,
    out_ref, where_ref, own_ref,
    emb, unit, ids_v, order_v, slot_v, size_v, sems,
):
    rows, depth = emb.shape
    part = rows // IN_PARTS
    owners, tiles = out_ref.shape[0], depth // LANES
    clusters = 2 * owners
    small = [
        pltpu.make_async_copy(source, target, sems.at[k])
        for k, (source, target) in enumerate(
            ((id_ref, ids_v), (slot_ref, slot_v), (order_ref, order_v), (size_ref, size_v))
        )
    ]
    large = [
        pltpu.make_async_copy(
            emb_ref.at[pl.ds(k * part, part)], emb.at[pl.ds(k * part, part)], sems.at[4 + k]
        )
        for k in range(IN_PARTS)
    ]
    for copy in small + large:
        copy.start()
    for copy in small:
        copy.wait()
    ids = ids_v[...]
    order = order_v[...]
    slots = slot_v[...]
    sizes = size_v[...]
    slot_of = chunk_slot(table_lookup(ids, slots).astype(jnp.int32), owners)
    size_of = table_lookup(ids, sizes).astype(jnp.int32)
    where_ref[...] = slot_of
    code = jnp.where(order < size_of, order + 1, 0).astype(jnp.float32)
    hit = iota((clusters, rows), 0) == slot_of
    rank = jnp.sum(jnp.where(hit, code, 0.0), axis=1, keepdims=True)
    coded = jnp.broadcast_to(rank, (clusters, LANES)).astype(jnp.bfloat16)
    out_ref[:, tiles] = coded.reshape(owners, 2, LANES)
    first_slot = lax.axis_index("dev") * 2
    size0 = jnp.sum(jnp.where(slots == first_slot, sizes, 0), axis=1, keepdims=True)
    size1 = jnp.sum(jnp.where(slots == first_slot + 1, sizes, 0), axis=1, keepdims=True)
    own_ref[...] = jnp.where(iota((1, LANES), 1) == 0, size0, size1)
    pick = hit.astype(jnp.bfloat16)
    for k, copy in enumerate(large):
        copy.wait()
        values = emb[k * part : (k + 1) * part]
        squares_sum = jnp.sum(values * values, axis=1, keepdims=True)
        unit[k * part : (k + 1) * part] = (
            values * lax.rsqrt(squares_sum + norm_eps)
        ).astype(jnp.bfloat16)
    for c in range(0, tiles, 2):
        placed = jnp.dot(
            pick, unit[:, c * LANES : (c + 2) * LANES], preferred_element_type=jnp.float32
        ).astype(jnp.bfloat16)
        out_ref[:, c] = placed[:, :LANES].reshape(owners, 2, LANES)
        out_ref[:, c + 1] = placed[:, LANES:].reshape(owners, 2, LANES)


def best_kernel(got_ref, own_ref, best_ref, mean_ref, spread_ref):
    sources, tiles = got_ref.shape[0], got_ref.shape[1] - 1
    rows = 2 * sources
    similar = jnp.zeros((rows, rows), jnp.float32)
    for q in range(0, tiles, STEP):
        unit = jnp.concatenate(
            [got_ref[:, c].reshape(rows, LANES) for c in range(q, q + STEP)], axis=1
        )
        similar += lax.dot_general(
            unit, unit, (((1,), (1,)), ((), ())), preferred_element_type=jnp.float32
        )
    coded = got_ref[:, tiles].reshape(rows, LANES)
    rank_col = coded.astype(jnp.float32)[:, :1]
    first = (iota((8, LANES), 1) == 0).astype(jnp.bfloat16)
    rank_row = lax.dot_general(
        first, coded, (((1,), (1,)), ((), ())), preferred_element_type=jnp.float32
    )[:1]
    same = ((iota((rows, rows), 0) ^ iota((rows, rows), 1)) & 1) == 0
    allowed = same & (rank_row > 0.0) & (rank_row < rank_col)
    best = jnp.max(jnp.where(allowed, similar, -1.0), axis=1, keepdims=True)
    spread_ref[...] = jnp.broadcast_to(best, spread_ref.shape)
    live_col = jnp.broadcast_to(rank_col, spread_ref.shape) > 0.0
    summed = jnp.where(live_col, spread_ref[...], 0.0)
    odd = (iota(spread_ref.shape, 0) & 1) == 1
    lane = iota((1, LANES), 1)
    total = jnp.where(
        lane == 0,
        jnp.sum(jnp.where(odd, 0.0, summed), axis=0, keepdims=True),
        jnp.sum(jnp.where(odd, summed, 0.0), axis=0, keepdims=True),
    )
    even_best = spread_ref[pl.ds(0, sources, stride=2), :]
    odd_best = spread_ref[pl.ds(1, sources, stride=2), :]
    best_ref[...] = jnp.where(iota((sources, LANES), 1) == 0, even_best, odd_best)
    mean_ref[...] = (total / own_ref[...].astype(jnp.float32))[:, : mean_ref.shape[1]]


def pick_kernel(back_ref, where_ref, best_ref, keep_ref):
    slot_of = where_ref[...]
    back = back_ref[...]
    owners = iota((back.shape[0], slot_of.shape[1]), 0)
    from_even = jnp.where(owners * 2 == slot_of, back[:, :1], 0.0)
    from_odd = jnp.where(owners * 2 + 1 == slot_of, back[:, 1:2], 0.0)
    best = jnp.sum(from_even + from_odd, axis=0, keepdims=True)
    best_ref[...] = best
    keep_ref[...] = (best < cutoff).astype(jnp.int32)


def body(embeddings, cluster_id, member_order, cluster_slot, cluster_size):
    devices = lax.axis_size("dev")
    rows, depth = embeddings.shape
    clusters = cluster_slot.shape[0]
    tiles = depth // LANES + 1
    sources = (
        embeddings,
        cluster_id.reshape(1, rows),
        member_order.reshape(1, rows),
        cluster_slot.reshape(1, clusters),
        cluster_size.reshape(1, clusters),
    )
    payload, place, own = pl.pallas_call(
        place_kernel,
        out_shape=(
            jax.ShapeDtypeStruct((devices, tiles, 2, LANES), jnp.bfloat16),
            jax.ShapeDtypeStruct((1, rows), jnp.int32),
            jax.ShapeDtypeStruct((1, LANES), jnp.int32),
        ),
        in_specs=[pl.BlockSpec(memory_space=pltpu.HBM)] * len(sources),
        scratch_shapes=[
            pltpu.VMEM((rows, depth), jnp.float32),
            pltpu.VMEM((rows, depth), jnp.bfloat16),
            pltpu.VMEM((1, rows), jnp.int32),
            pltpu.VMEM((1, rows), jnp.int32),
            pltpu.VMEM((1, clusters), jnp.int32),
            pltpu.VMEM((1, clusters), jnp.int32),
            pltpu.SemaphoreType.DMA((4 + IN_PARTS,)),
        ],
        name="place",
        compiler_params=pltpu.CompilerParams(vmem_limit_bytes=KERNEL_VMEM),
    )(*[pltpu.with_memory_space_constraint(x, pltpu.HBM) for x in sources])
    got = exchange(payload, devices)
    best, mean = pl.pallas_call(
        best_kernel,
        out_shape=(
            jax.ShapeDtypeStruct((devices, LANES), jnp.float32),
            jax.ShapeDtypeStruct((1, 2), jnp.float32),
        ),
        scratch_shapes=[
            pltpu.VMEM((clusters, LANES), jnp.float32),
        ],
        name="best",
        compiler_params=pltpu.CompilerParams(vmem_limit_bytes=KERNEL_VMEM),
    )(got, own)
    back = exchange(best.reshape(devices, 1, LANES), devices).reshape(devices, LANES)
    row_best, keep = pl.pallas_call(
        pick_kernel,
        out_shape=(
            jax.ShapeDtypeStruct((1, rows), jnp.float32),
            jax.ShapeDtypeStruct((1, rows), jnp.int32),
        ),
        name="pick",
        compiler_params=pltpu.CompilerParams(vmem_limit_bytes=KERNEL_VMEM),
    )(back, place)
    return (row_best.reshape(rows), keep.reshape(rows), mean.reshape(2))


def solution(mesh):
    placed = (P(("rep", "dev"), None), P(("rep", "dev")), P(("rep", "dev")), P("rep"), P("rep"))
    return jax.shard_map(
        body,
        mesh=mesh,
        in_specs=placed,
        out_specs=(P(("rep", "dev")), P(("rep", "dev")), P(("rep", "dev"))),
        check_vma=False,
    )
```

```python
import jax
import jax.numpy as jnp
from jax import lax
from jax.experimental import pallas as pl
from jax.experimental.pallas import tpu as pltpu
from jax.sharding import PartitionSpec as P

CAP = 128
LANES = 128
KERNEL_VMEM = 24 * 2**20
STEP = 8
IN_PARTS = 8

norm_eps = 1e-06
cutoff = 0.8


def iota(shape, axis):
    return lax.broadcasted_iota(jnp.int32, shape, axis)


def table_lookup(cluster_row, table_row):
    clusters = table_row.shape[1]
    hit = (iota((clusters, cluster_row.shape[1]), 0) == cluster_row).astype(jnp.bfloat16)
    table = jnp.broadcast_to(table_row.astype(jnp.bfloat16), (8, clusters))
    return jnp.dot(table, hit, preferred_element_type=jnp.float32)[:1]


def chunk_of(device, devices):
    y, x, z = ((device >> 5) + 1) & 3, ((device >> 3) + 1) & 3, (device * 3) & 7
    y, x = ((y & 1) << 1) | (y >> 1), ((x & 1) << 1) | (x >> 1)
    return devices - 1 - ((y << 5) | (x << 3) | z)


def chunk_slot(slot, devices):
    return chunk_of(slot >> 1, devices) * 2 + (slot & 1)


def exchange(x, devices):
    order = sorted(range(devices), key=lambda device: chunk_of(device, devices))
    return lax.all_to_all(
        x, "dev", split_axis=0, concat_axis=0, axis_index_groups=[order], tiled=True
    )


def place_kernel(
    emb_ref, id_ref, order_ref, slot_ref, size_ref,
    out_ref, where_ref, own_ref,
    emb, unit, ids_v, order_v, slot_v, size_v, sems,
):
    rows, depth = emb.shape
    part = rows // IN_PARTS
    owners, tiles = out_ref.shape[0], depth // LANES
    clusters = 2 * owners
    small = [
        pltpu.make_async_copy(source, target, sems.at[k])
        for k, (source, target) in enumerate(
            ((id_ref, ids_v), (slot_ref, slot_v), (order_ref, order_v), (size_ref, size_v))
        )
    ]
    large = [
        pltpu.make_async_copy(
            emb_ref.at[pl.ds(k * part, part)], emb.at[pl.ds(k * part, part)], sems.at[4 + k]
        )
        for k in range(IN_PARTS)
    ]
    for copy in small + large:
        copy.start()
    for copy in small:
        copy.wait()
    ids = ids_v[...]
    order = order_v[...]
    slots = slot_v[...]
    sizes = size_v[...]
    slot_of = chunk_slot(table_lookup(ids, slots).astype(jnp.int32), owners)
    size_of = table_lookup(ids, sizes).astype(jnp.int32)
    where_ref[...] = slot_of
    code = jnp.where(order < size_of, order + 1, 0).astype(jnp.float32)
    hit = iota((clusters, rows), 0) == slot_of
    rank = jnp.sum(jnp.where(hit, code, 0.0), axis=1, keepdims=True)
    coded = jnp.broadcast_to(rank, (clusters, LANES)).astype(jnp.bfloat16)
    out_ref[:, tiles] = coded.reshape(owners, 2, LANES)
    first_slot = lax.axis_index("dev") * 2
    size0 = jnp.sum(jnp.where(slots == first_slot, sizes, 0), axis=1, keepdims=True)
    size1 = jnp.sum(jnp.where(slots == first_slot + 1, sizes, 0), axis=1, keepdims=True)
    own_ref[...] = jnp.where(iota((1, LANES), 1) == 0, size0, size1)
    pick = hit.astype(jnp.bfloat16)
    for k, copy in enumerate(large):
        copy.wait()
        values = emb[k * part : (k + 1) * part]
        squares_sum = jnp.sum(values * values, axis=1, keepdims=True)
        unit[k * part : (k + 1) * part] = (
            values * lax.rsqrt(squares_sum + norm_eps)
        ).astype(jnp.bfloat16)
    for c in range(0, tiles, 2):
        placed = jnp.dot(
            pick, unit[:, c * LANES : (c + 2) * LANES], preferred_element_type=jnp.float32
        ).astype(jnp.bfloat16)
        out_ref[:, c] = placed[:, :LANES].reshape(owners, 2, LANES)
        out_ref[:, c + 1] = placed[:, LANES:].reshape(owners, 2, LANES)


def best_kernel(got_ref, own_ref, best_ref, mean_ref, spread_ref):
    sources, tiles = got_ref.shape[0], got_ref.shape[1] - 1
    rows = 2 * sources
    similar = jnp.zeros((rows, rows), jnp.float32)
    for q in range(0, tiles, STEP):
        unit = jnp.concatenate(
            [got_ref[:, c].reshape(rows, LANES) for c in range(q, q + STEP)], axis=1
        )
        similar += lax.dot_general(
            unit, unit, (((1,), (1,)), ((), ())), preferred_element_type=jnp.float32
        )
    coded = got_ref[:, tiles].reshape(rows, LANES)
    rank_col = coded.astype(jnp.float32)[:, :1]
    first = (iota((8, LANES), 1) == 0).astype(jnp.bfloat16)
    rank_row = lax.dot_general(
        first, coded, (((1,), (1,)), ((), ())), preferred_element_type=jnp.float32
    )[:1]
    same = ((iota((rows, rows), 0) ^ iota((rows, rows), 1)) & 1) == 0
    allowed = same & (rank_row > 0.0) & (rank_row < rank_col)
    best = jnp.max(jnp.where(allowed, similar, -1.0), axis=1, keepdims=True)
    spread_ref[...] = jnp.broadcast_to(best, spread_ref.shape)
    live_col = jnp.broadcast_to(rank_col, spread_ref.shape) > 0.0
    summed = jnp.where(live_col, spread_ref[...], 0.0)
    odd = (iota(spread_ref.shape, 0) & 1) == 1
    lane = iota((1, LANES), 1)
    total = jnp.where(
        lane == 0,
        jnp.sum(jnp.where(odd, 0.0, summed), axis=0, keepdims=True),
        jnp.sum(jnp.where(odd, summed, 0.0), axis=0, keepdims=True),
    )
    even_best = spread_ref[pl.ds(0, sources, stride=2), :]
    odd_best = spread_ref[pl.ds(1, sources, stride=2), :]
    best_ref[...] = jnp.where(iota((sources, LANES), 1) == 0, even_best, odd_best)
    mean_ref[...] = (total / own_ref[...].astype(jnp.float32))[:, : mean_ref.shape[1]]


def pick_kernel(back_ref, where_ref, best_ref, keep_ref):
    slot_of = where_ref[...]
    back = back_ref[...]
    owners = iota((back.shape[0], slot_of.shape[1]), 0)
    from_even = jnp.where(owners * 2 == slot_of, back[:, :1], 0.0)
    from_odd = jnp.where(owners * 2 + 1 == slot_of, back[:, 1:2], 0.0)
    best = jnp.sum(from_even + from_odd, axis=0, keepdims=True)
    best_ref[...] = best
    keep_ref[...] = (best < cutoff).astype(jnp.int32)


def body(embeddings, cluster_id, member_order, cluster_slot, cluster_size):
    devices = lax.axis_size("dev")
    rows, depth = embeddings.shape
    clusters = cluster_slot.shape[0]
    tiles = depth // LANES + 1
    sources = (
        embeddings,
        cluster_id.reshape(1, rows),
        member_order.reshape(1, rows),
        cluster_slot.reshape(1, clusters),
        cluster_size.reshape(1, clusters),
    )
    payload, place, own = pl.pallas_call(
        place_kernel,
        out_shape=(
            jax.ShapeDtypeStruct((devices, tiles, 2, LANES), jnp.bfloat16),
            jax.ShapeDtypeStruct((1, rows), jnp.int32),
            jax.ShapeDtypeStruct((1, LANES), jnp.int32),
        ),
        in_specs=[pl.BlockSpec(memory_space=pltpu.HBM)] * len(sources),
        scratch_shapes=[
            pltpu.VMEM((rows, depth), jnp.float32),
            pltpu.VMEM((rows, depth), jnp.bfloat16),
            pltpu.VMEM((1, rows), jnp.int32),
            pltpu.VMEM((1, rows), jnp.int32),
            pltpu.VMEM((1, clusters), jnp.int32),
            pltpu.VMEM((1, clusters), jnp.int32),
            pltpu.SemaphoreType.DMA((4 + IN_PARTS,)),
        ],
        name="place",
        compiler_params=pltpu.CompilerParams(vmem_limit_bytes=KERNEL_VMEM),
    )(*[pltpu.with_memory_space_constraint(x, pltpu.HBM) for x in sources])
    got = exchange(payload, devices)
    best, mean = pl.pallas_call(
        best_kernel,
        out_shape=(
            jax.ShapeDtypeStruct((devices, LANES), jnp.float32),
            jax.ShapeDtypeStruct((1, 2), jnp.float32),
        ),
        scratch_shapes=[
            pltpu.VMEM((clusters, LANES), jnp.float32),
        ],
        name="best",
        compiler_params=pltpu.CompilerParams(vmem_limit_bytes=KERNEL_VMEM),
    )(got, own)
    back = exchange(best.reshape(devices, 1, LANES), devices).reshape(devices, LANES)
    row_best, keep = pl.pallas_call(
        pick_kernel,
        out_shape=(
            jax.ShapeDtypeStruct((1, rows), jnp.float32),
            jax.ShapeDtypeStruct((1, rows), jnp.int32),
        ),
        name="pick",
        compiler_params=pltpu.CompilerParams(vmem_limit_bytes=KERNEL_VMEM),
    )(back, place)
    return (row_best.reshape(rows), keep.reshape(rows), mean.reshape(2))


def solution(mesh):
    placed = (P(("rep", "dev"), None), P(("rep", "dev")), P(("rep", "dev")), P("rep"), P("rep"))
    return jax.shard_map(
        body,
        mesh=mesh,
        in_specs=placed,
        out_specs=(P(("rep", "dev")), P(("rep", "dev")), P(("rep", "dev"))),
        check_vma=False,
    )
```

```python
import jax
import jax.numpy as jnp
from jax import lax
from jax.experimental import pallas as pl
from jax.experimental.pallas import tpu as pltpu
from jax.sharding import PartitionSpec as P

CAP = 128
LANES = 128
KERNEL_VMEM = 24 * 2**20
STEP = 8
IN_PARTS = 8

norm_eps = 1e-06
cutoff = 0.8


def iota(shape, axis):
    return lax.broadcasted_iota(jnp.int32, shape, axis)


def table_lookup(cluster_row, table_row):
    clusters = table_row.shape[1]
    hit = (iota((clusters, cluster_row.shape[1]), 0) == cluster_row).astype(jnp.bfloat16)
    table = jnp.broadcast_to(table_row.astype(jnp.bfloat16), (8, clusters))
    return jnp.dot(table, hit, preferred_element_type=jnp.float32)[:1]


def chunk_of(device, devices):
    y, x, z = ((device >> 5) + 1) & 3, ((device >> 3) + 1) & 3, (device * 3) & 7
    y, x = ((y & 1) << 1) | (y >> 1), ((x & 1) << 1) | (x >> 1)
    return devices - 1 - ((z << 4) | (y << 2) | x)


def chunk_slot(slot, devices):
    return chunk_of(slot >> 1, devices) * 2 + (slot & 1)


def exchange(x, devices):
    order = sorted(range(devices), key=lambda device: chunk_of(device, devices))
    return lax.all_to_all(
        x, "dev", split_axis=0, concat_axis=0, axis_index_groups=[order], tiled=True
    )


def place_kernel(
    emb_ref, id_ref, order_ref, slot_ref, size_ref,
    out_ref, where_ref, own_ref,
    emb, unit, ids_v, order_v, slot_v, size_v, sems,
):
    rows, depth = emb.shape
    part = rows // IN_PARTS
    owners, tiles = out_ref.shape[0], depth // LANES
    clusters = 2 * owners
    small = [
        pltpu.make_async_copy(source, target, sems.at[k])
        for k, (source, target) in enumerate(
            ((id_ref, ids_v), (slot_ref, slot_v), (order_ref, order_v), (size_ref, size_v))
        )
    ]
    large = [
        pltpu.make_async_copy(
            emb_ref.at[pl.ds(k * part, part)], emb.at[pl.ds(k * part, part)], sems.at[4 + k]
        )
        for k in range(IN_PARTS)
    ]
    for copy in small + large:
        copy.start()
    for copy in small:
        copy.wait()
    ids = ids_v[...]
    order = order_v[...]
    slots = slot_v[...]
    sizes = size_v[...]
    slot_of = chunk_slot(table_lookup(ids, slots).astype(jnp.int32), owners)
    size_of = table_lookup(ids, sizes).astype(jnp.int32)
    where_ref[...] = slot_of
    code = jnp.where(order < size_of, order + 1, 0).astype(jnp.float32)
    hit = iota((clusters, rows), 0) == slot_of
    rank = jnp.sum(jnp.where(hit, code, 0.0), axis=1, keepdims=True)
    coded = jnp.broadcast_to(rank, (clusters, LANES)).astype(jnp.bfloat16)
    out_ref[:, tiles] = coded.reshape(owners, 2, LANES)
    first_slot = lax.axis_index("dev") * 2
    size0 = jnp.sum(jnp.where(slots == first_slot, sizes, 0), axis=1, keepdims=True)
    size1 = jnp.sum(jnp.where(slots == first_slot + 1, sizes, 0), axis=1, keepdims=True)
    own_ref[...] = jnp.where(iota((1, LANES), 1) == 0, size0, size1)
    pick = hit.astype(jnp.bfloat16)
    for k, copy in enumerate(large):
        copy.wait()
        values = emb[k * part : (k + 1) * part]
        squares_sum = jnp.sum(values * values, axis=1, keepdims=True)
        unit[k * part : (k + 1) * part] = (
            values * lax.rsqrt(squares_sum + norm_eps)
        ).astype(jnp.bfloat16)
    for c in range(0, tiles, 2):
        placed = jnp.dot(
            pick, unit[:, c * LANES : (c + 2) * LANES], preferred_element_type=jnp.float32
        ).astype(jnp.bfloat16)
        out_ref[:, c] = placed[:, :LANES].reshape(owners, 2, LANES)
        out_ref[:, c + 1] = placed[:, LANES:].reshape(owners, 2, LANES)


def best_kernel(got_ref, own_ref, best_ref, mean_ref, spread_ref):
    sources, tiles = got_ref.shape[0], got_ref.shape[1] - 1
    rows = 2 * sources
    similar = jnp.zeros((rows, rows), jnp.float32)
    for q in range(0, tiles, STEP):
        unit = jnp.concatenate(
            [got_ref[:, c].reshape(rows, LANES) for c in range(q, q + STEP)], axis=1
        )
        similar += lax.dot_general(
            unit, unit, (((1,), (1,)), ((), ())), preferred_element_type=jnp.float32
        )
    coded = got_ref[:, tiles].reshape(rows, LANES)
    rank_col = coded.astype(jnp.float32)[:, :1]
    first = (iota((8, LANES), 1) == 0).astype(jnp.bfloat16)
    rank_row = lax.dot_general(
        first, coded, (((1,), (1,)), ((), ())), preferred_element_type=jnp.float32
    )[:1]
    same = ((iota((rows, rows), 0) ^ iota((rows, rows), 1)) & 1) == 0
    allowed = same & (rank_row > 0.0) & (rank_row < rank_col)
    best = jnp.max(jnp.where(allowed, similar, -1.0), axis=1, keepdims=True)
    spread_ref[...] = jnp.broadcast_to(best, spread_ref.shape)
    live_col = jnp.broadcast_to(rank_col, spread_ref.shape) > 0.0
    summed = jnp.where(live_col, spread_ref[...], 0.0)
    odd = (iota(spread_ref.shape, 0) & 1) == 1
    lane = iota((1, LANES), 1)
    total = jnp.where(
        lane == 0,
        jnp.sum(jnp.where(odd, 0.0, summed), axis=0, keepdims=True),
        jnp.sum(jnp.where(odd, summed, 0.0), axis=0, keepdims=True),
    )
    even_best = spread_ref[pl.ds(0, sources, stride=2), :]
    odd_best = spread_ref[pl.ds(1, sources, stride=2), :]
    best_ref[...] = jnp.where(iota((sources, LANES), 1) == 0, even_best, odd_best)
    mean_ref[...] = (total / own_ref[...].astype(jnp.float32))[:, : mean_ref.shape[1]]


def pick_kernel(back_ref, where_ref, best_ref, keep_ref):
    slot_of = where_ref[...]
    back = back_ref[...]
    owners = iota((back.shape[0], slot_of.shape[1]), 0)
    from_even = jnp.where(owners * 2 == slot_of, back[:, :1], 0.0)
    from_odd = jnp.where(owners * 2 + 1 == slot_of, back[:, 1:2], 0.0)
    best = jnp.sum(from_even + from_odd, axis=0, keepdims=True)
    best_ref[...] = best
    keep_ref[...] = (best < cutoff).astype(jnp.int32)


def body(embeddings, cluster_id, member_order, cluster_slot, cluster_size):
    devices = lax.axis_size("dev")
    rows, depth = embeddings.shape
    clusters = cluster_slot.shape[0]
    tiles = depth // LANES + 1
    sources = (
        embeddings,
        cluster_id.reshape(1, rows),
        member_order.reshape(1, rows),
        cluster_slot.reshape(1, clusters),
        cluster_size.reshape(1, clusters),
    )
    payload, place, own = pl.pallas_call(
        place_kernel,
        out_shape=(
            jax.ShapeDtypeStruct((devices, tiles, 2, LANES), jnp.bfloat16),
            jax.ShapeDtypeStruct((1, rows), jnp.int32),
            jax.ShapeDtypeStruct((1, LANES), jnp.int32),
        ),
        in_specs=[pl.BlockSpec(memory_space=pltpu.HBM)] * len(sources),
        scratch_shapes=[
            pltpu.VMEM((rows, depth), jnp.float32),
            pltpu.VMEM((rows, depth), jnp.bfloat16),
            pltpu.VMEM((1, rows), jnp.int32),
            pltpu.VMEM((1, rows), jnp.int32),
            pltpu.VMEM((1, clusters), jnp.int32),
            pltpu.VMEM((1, clusters), jnp.int32),
            pltpu.SemaphoreType.DMA((4 + IN_PARTS,)),
        ],
        name="place",
        compiler_params=pltpu.CompilerParams(vmem_limit_bytes=KERNEL_VMEM),
    )(*[pltpu.with_memory_space_constraint(x, pltpu.HBM) for x in sources])
    got = exchange(payload, devices)
    best, mean = pl.pallas_call(
        best_kernel,
        out_shape=(
            jax.ShapeDtypeStruct((devices, LANES), jnp.float32),
            jax.ShapeDtypeStruct((1, 2), jnp.float32),
        ),
        scratch_shapes=[
            pltpu.VMEM((clusters, LANES), jnp.float32),
        ],
        name="best",
        compiler_params=pltpu.CompilerParams(vmem_limit_bytes=KERNEL_VMEM),
    )(got, own)
    back = exchange(best.reshape(devices, 1, LANES), devices).reshape(devices, LANES)
    row_best, keep = pl.pallas_call(
        pick_kernel,
        out_shape=(
            jax.ShapeDtypeStruct((1, rows), jnp.float32),
            jax.ShapeDtypeStruct((1, rows), jnp.int32),
        ),
        name="pick",
        compiler_params=pltpu.CompilerParams(vmem_limit_bytes=KERNEL_VMEM),
    )(back, place)
    return (row_best.reshape(rows), keep.reshape(rows), mean.reshape(2))


def solution(mesh):
    placed = (P(("rep", "dev"), None), P(("rep", "dev")), P(("rep", "dev")), P("rep"), P("rep"))
    return jax.shard_map(
        body,
        mesh=mesh,
        in_specs=placed,
        out_specs=(P(("rep", "dev")), P(("rep", "dev")), P(("rep", "dev"))),
        check_vma=False,
    )
```

```python
import jax
import jax.numpy as jnp
from jax import lax
from jax.experimental import pallas as pl
from jax.experimental.pallas import tpu as pltpu
from jax.sharding import PartitionSpec as P

CAP = 128
LANES = 128
KERNEL_VMEM = 24 * 2**20
STEP = 8
IN_PARTS = 8

norm_eps = 1e-06
cutoff = 0.8


def iota(shape, axis):
    return lax.broadcasted_iota(jnp.int32, shape, axis)


def table_lookup(cluster_row, table_row):
    clusters = table_row.shape[1]
    hit = (iota((clusters, cluster_row.shape[1]), 0) == cluster_row).astype(jnp.bfloat16)
    table = jnp.broadcast_to(table_row.astype(jnp.bfloat16), (8, clusters))
    return jnp.dot(table, hit, preferred_element_type=jnp.float32)[:1]


def chunk_of(device, devices):
    y, x, z = ((device >> 5) + 1) & 3, ((device >> 3) + 1) & 3, (device * 3) & 7
    y, x = ((y & 1) << 1) | (y >> 1), ((x & 1) << 1) | (x >> 1)
    return devices - 1 - ((y << 5) | (z << 2) | x)


def chunk_slot(slot, devices):
    return chunk_of(slot >> 1, devices) * 2 + (slot & 1)


def exchange(x, devices):
    order = sorted(range(devices), key=lambda device: chunk_of(device, devices))
    return lax.all_to_all(
        x, "dev", split_axis=0, concat_axis=0, axis_index_groups=[order], tiled=True
    )


def place_kernel(
    emb_ref, id_ref, order_ref, slot_ref, size_ref,
    out_ref, where_ref, own_ref,
    emb, unit, ids_v, order_v, slot_v, size_v, sems,
):
    rows, depth = emb.shape
    part = rows // IN_PARTS
    owners, tiles = out_ref.shape[0], depth // LANES
    clusters = 2 * owners
    small = [
        pltpu.make_async_copy(source, target, sems.at[k])
        for k, (source, target) in enumerate(
            ((id_ref, ids_v), (slot_ref, slot_v), (order_ref, order_v), (size_ref, size_v))
        )
    ]
    large = [
        pltpu.make_async_copy(
            emb_ref.at[pl.ds(k * part, part)], emb.at[pl.ds(k * part, part)], sems.at[4 + k]
        )
        for k in range(IN_PARTS)
    ]
    for copy in small + large:
        copy.start()
    for copy in small:
        copy.wait()
    ids = ids_v[...]
    order = order_v[...]
    slots = slot_v[...]
    sizes = size_v[...]
    slot_of = chunk_slot(table_lookup(ids, slots).astype(jnp.int32), owners)
    size_of = table_lookup(ids, sizes).astype(jnp.int32)
    where_ref[...] = slot_of
    code = jnp.where(order < size_of, order + 1, 0).astype(jnp.float32)
    hit = iota((clusters, rows), 0) == slot_of
    rank = jnp.sum(jnp.where(hit, code, 0.0), axis=1, keepdims=True)
    coded = jnp.broadcast_to(rank, (clusters, LANES)).astype(jnp.bfloat16)
    out_ref[:, tiles] = coded.reshape(owners, 2, LANES)
    first_slot = lax.axis_index("dev") * 2
    size0 = jnp.sum(jnp.where(slots == first_slot, sizes, 0), axis=1, keepdims=True)
    size1 = jnp.sum(jnp.where(slots == first_slot + 1, sizes, 0), axis=1, keepdims=True)
    own_ref[...] = jnp.where(iota((1, LANES), 1) == 0, size0, size1)
    pick = hit.astype(jnp.bfloat16)
    for k, copy in enumerate(large):
        copy.wait()
        values = emb[k * part : (k + 1) * part]
        squares_sum = jnp.sum(values * values, axis=1, keepdims=True)
        unit[k * part : (k + 1) * part] = (
            values * lax.rsqrt(squares_sum + norm_eps)
        ).astype(jnp.bfloat16)
    for c in range(0, tiles, 2):
        placed = jnp.dot(
            pick, unit[:, c * LANES : (c + 2) * LANES], preferred_element_type=jnp.float32
        ).astype(jnp.bfloat16)
        out_ref[:, c] = placed[:, :LANES].reshape(owners, 2, LANES)
        out_ref[:, c + 1] = placed[:, LANES:].reshape(owners, 2, LANES)


def best_kernel(got_ref, own_ref, best_ref, mean_ref, spread_ref):
    sources, tiles = got_ref.shape[0], got_ref.shape[1] - 1
    rows = 2 * sources
    similar = jnp.zeros((rows, rows), jnp.float32)
    for q in range(0, tiles, STEP):
        unit = jnp.concatenate(
            [got_ref[:, c].reshape(rows, LANES) for c in range(q, q + STEP)], axis=1
        )
        similar += lax.dot_general(
            unit, unit, (((1,), (1,)), ((), ())), preferred_element_type=jnp.float32
        )
    coded = got_ref[:, tiles].reshape(rows, LANES)
    rank_col = coded.astype(jnp.float32)[:, :1]
    first = (iota((8, LANES), 1) == 0).astype(jnp.bfloat16)
    rank_row = lax.dot_general(
        first, coded, (((1,), (1,)), ((), ())), preferred_element_type=jnp.float32
    )[:1]
    same = ((iota((rows, rows), 0) ^ iota((rows, rows), 1)) & 1) == 0
    allowed = same & (rank_row > 0.0) & (rank_row < rank_col)
    best = jnp.max(jnp.where(allowed, similar, -1.0), axis=1, keepdims=True)
    spread_ref[...] = jnp.broadcast_to(best, spread_ref.shape)
    live_col = jnp.broadcast_to(rank_col, spread_ref.shape) > 0.0
    summed = jnp.where(live_col, spread_ref[...], 0.0)
    odd = (iota(spread_ref.shape, 0) & 1) == 1
    lane = iota((1, LANES), 1)
    total = jnp.where(
        lane == 0,
        jnp.sum(jnp.where(odd, 0.0, summed), axis=0, keepdims=True),
        jnp.sum(jnp.where(odd, summed, 0.0), axis=0, keepdims=True),
    )
    even_best = spread_ref[pl.ds(0, sources, stride=2), :]
    odd_best = spread_ref[pl.ds(1, sources, stride=2), :]
    best_ref[...] = jnp.where(iota((sources, LANES), 1) == 0, even_best, odd_best)
    mean_ref[...] = (total / own_ref[...].astype(jnp.float32))[:, : mean_ref.shape[1]]


def pick_kernel(back_ref, where_ref, best_ref, keep_ref):
    slot_of = where_ref[...]
    back = back_ref[...]
    owners = iota((back.shape[0], slot_of.shape[1]), 0)
    from_even = jnp.where(owners * 2 == slot_of, back[:, :1], 0.0)
    from_odd = jnp.where(owners * 2 + 1 == slot_of, back[:, 1:2], 0.0)
    best = jnp.sum(from_even + from_odd, axis=0, keepdims=True)
    best_ref[...] = best
    keep_ref[...] = (best < cutoff).astype(jnp.int32)


def body(embeddings, cluster_id, member_order, cluster_slot, cluster_size):
    devices = lax.axis_size("dev")
    rows, depth = embeddings.shape
    clusters = cluster_slot.shape[0]
    tiles = depth // LANES + 1
    sources = (
        embeddings,
        cluster_id.reshape(1, rows),
        member_order.reshape(1, rows),
        cluster_slot.reshape(1, clusters),
        cluster_size.reshape(1, clusters),
    )
    payload, place, own = pl.pallas_call(
        place_kernel,
        out_shape=(
            jax.ShapeDtypeStruct((devices, tiles, 2, LANES), jnp.bfloat16),
            jax.ShapeDtypeStruct((1, rows), jnp.int32),
            jax.ShapeDtypeStruct((1, LANES), jnp.int32),
        ),
        in_specs=[pl.BlockSpec(memory_space=pltpu.HBM)] * len(sources),
        scratch_shapes=[
            pltpu.VMEM((rows, depth), jnp.float32),
            pltpu.VMEM((rows, depth), jnp.bfloat16),
            pltpu.VMEM((1, rows), jnp.int32),
            pltpu.VMEM((1, rows), jnp.int32),
            pltpu.VMEM((1, clusters), jnp.int32),
            pltpu.VMEM((1, clusters), jnp.int32),
            pltpu.SemaphoreType.DMA((4 + IN_PARTS,)),
        ],
        name="place",
        compiler_params=pltpu.CompilerParams(vmem_limit_bytes=KERNEL_VMEM),
    )(*[pltpu.with_memory_space_constraint(x, pltpu.HBM) for x in sources])
    got = exchange(payload, devices)
    best, mean = pl.pallas_call(
        best_kernel,
        out_shape=(
            jax.ShapeDtypeStruct((devices, LANES), jnp.float32),
            jax.ShapeDtypeStruct((1, 2), jnp.float32),
        ),
        scratch_shapes=[
            pltpu.VMEM((clusters, LANES), jnp.float32),
        ],
        name="best",
        compiler_params=pltpu.CompilerParams(vmem_limit_bytes=KERNEL_VMEM),
    )(got, own)
    back = exchange(best.reshape(devices, 1, LANES), devices).reshape(devices, LANES)
    row_best, keep = pl.pallas_call(
        pick_kernel,
        out_shape=(
            jax.ShapeDtypeStruct((1, rows), jnp.float32),
            jax.ShapeDtypeStruct((1, rows), jnp.int32),
        ),
        name="pick",
        compiler_params=pltpu.CompilerParams(vmem_limit_bytes=KERNEL_VMEM),
    )(back, place)
    return (row_best.reshape(rows), keep.reshape(rows), mean.reshape(2))


def solution(mesh):
    placed = (P(("rep", "dev"), None), P(("rep", "dev")), P(("rep", "dev")), P("rep"), P("rep"))
    return jax.shard_map(
        body,
        mesh=mesh,
        in_specs=placed,
        out_specs=(P(("rep", "dev")), P(("rep", "dev")), P(("rep", "dev"))),
        check_vma=False,
    )
```
